256 devices in a mesh: runs: 4 (over y, x), gx: 64 (over z, core).
Axes of the slice: x: 2, y: 2, z: 32, core: 2. Of those that a mesh axis runs over, the one named last changes fastest.
The devices are a block of a 4x8x32 slice.
Arguments:
- potential: float32 [512, 512, 512], P(('runs', 'gx')), parts along dimension 0, may hold values from -3 to 3
Outputs:
- second_potential: float32 [512, 512, 512], P(('runs', 'gx')), parts along dimension 0
- norms: float32 [8], P('runs'), parts along dimension 0
The draws below stay inside these ranges and needn't reach their ends.
There are 4 independent parts, one for each index of `runs`. The reference program is written for one: setup_inputs(seed, part) draws one part's arguments, and reference() takes and returns one part's arrays. A program takes and returns all parts, laid end to end along the dimension named above; each array names one. Nothing has to cross between parts.
All inputs are finite; a program needn't handle non-finite values.
Results may differ from the reference program's by a relative error of at most 0.00015.
Values sent between devices are 32-bit elements; how exact they have to be, the bound alone decides.
No kernel may reach another device: no remote copies, remote signals or barrier semaphores. Data moves between devices by JAX's collectives and lax.ppermute only.
A program may use at most 256 MiB of HBM per device.

```python
import jax
import jax.numpy as jnp
from jax import lax

NY = 512
NZ = 512
LEVELS = 2
PRE = 1
POST = 1
COARSE = 4
CYCLES = 2
NX = 128


def steps_of(key, dims, split, least, high):
    level, own = 1.0, jax.random.fold_in(key, 6)
    for axis_at, parts in split:
        draws = jnp.exp(jax.random.uniform(jax.random.fold_in(own, axis_at), (parts,), jnp.float32, least / len(split), high / len(split)))
        level = level * jnp.repeat(draws, dims[axis_at] // parts).reshape([-1 if axis == axis_at else 1 for axis in range(len(dims))])
    return level


def scatter_about(stream_key, extent, width, limit, shards=(), held_as=jnp.bfloat16):
    factor_of = steps_of(stream_key, extent, shards, -0.22, 0.18) if shards else 1.0
    entries = jax.random.normal(stream_key, extent, jnp.float32) * width * factor_of
    return jnp.minimum(jnp.maximum(entries, -limit), limit).astype(held_as)


def setup_inputs(seed: int = 0, part: int = 0) -> dict:
    streams_of = jax.random.split(jax.random.key(seed), 2)
    part_splits = jax.random.split(jax.random.fold_in(streams_of[1], part), 2)
    potential = scatter_about(part_splits[0], (NX, NY, NZ), 0.5, 3.0, ((0, 64),), jnp.float32)
    return dict(potential=potential)


RELAX = 0.8

def wrap_pad(field):
    return jnp.concatenate([field[-1:], field, field[:1]], 0)

def shifted(field, offset, axis):
    return jnp.roll(field, -offset, axis)

def source_term(padded):
    center = padded[1:-1]
    upper = padded[2:]
    lower = padded[:-2]
    curve_xx = upper + lower - 2.0 * center
    curve_yy = shifted(center, 1, 1) + shifted(center, -1, 1) - 2.0 * center
    curve_zz = shifted(center, 1, 2) + shifted(center, -1, 2) - 2.0 * center
    cross_xy = (shifted(upper, 1, 1) - shifted(upper, -1, 1) - shifted(lower, 1, 1) + shifted(lower, -1, 1)) * 0.25
    cross_xz = (shifted(upper, 1, 2) - shifted(upper, -1, 2) - shifted(lower, 1, 2) + shifted(lower, -1, 2)) * 0.25
    plus_y = shifted(center, 1, 1)
    minus_y = shifted(center, -1, 1)
    cross_yz = (shifted(plus_y, 1, 2) - shifted(plus_y, -1, 2) - shifted(minus_y, 1, 2) + shifted(minus_y, -1, 2)) * 0.25
    return curve_xx * curve_yy - cross_xy * cross_xy + curve_xx * curve_zz - cross_xz * cross_xz + curve_yy * curve_zz - cross_yz * cross_yz

def operator(padded, spacing):
    center = padded[1:-1]
    beside_all = padded[2:] + padded[:-2]
    beside_all = beside_all + shifted(center, 1, 1) + shifted(center, -1, 1)
    beside_all = beside_all + shifted(center, 1, 2) + shifted(center, -1, 2)
    return (6.0 * center - beside_all) / spacing

def relax(padded, forcing, spacing):
    return padded[1:-1] + RELAX * spacing / 6.0 * (forcing - operator(padded, spacing))

def restrict(field):
    planes, rows, cols = field.shape
    blocks = field.reshape(planes // 2, 2, rows // 2, 2, cols // 2, 2)
    return lax.optimization_barrier(jnp.mean(blocks, axis=(1, 3, 5)))

def prolong(field):
    return jnp.repeat(jnp.repeat(jnp.repeat(field, 2, 0), 2, 1), 2, 2)

def smooth(field, forcing, spacing, count):
    for sweep_index in range(count):
        field = relax(wrap_pad(field), forcing, spacing)
    return field

def vcycle(field, forcing, level):
    spacing = float(4 ** level)
    if level == LEVELS - 1:
        return smooth(jnp.zeros_like(forcing), forcing, spacing, COARSE)
    field = smooth(field, forcing, spacing, PRE)
    residue = forcing - operator(wrap_pad(field), spacing)
    coarse_rhs = restrict(residue)
    correction = vcycle(jnp.zeros_like(coarse_rhs), coarse_rhs, level + 1)
    field = field + prolong(correction)
    return smooth(field, forcing, spacing, POST)

def reference(potential):
    source = source_term(wrap_pad(potential))
    forcing = -(source - jnp.mean(source))
    field = jnp.zeros_like(forcing)
    results = []
    for cycle_index in range(CYCLES):
        field = vcycle(field, forcing, 0)
        residue = forcing - operator(wrap_pad(field), 1.0)
        results.append(jnp.sqrt(jnp.mean(residue * residue)))
    return (field, jnp.stack(results))
```

```python
import functools

import jax
import jax.numpy as jnp
import numpy as np
from jax import lax
from jax.experimental import pallas as pl
from jax.experimental.pallas import tpu as pltpu
from jax.sharding import PartitionSpec as P

CYCLES = 2
COARSE = 4
RELAX = 0.8
KAPPA = RELAX / 6.0
COARSE_SCALE = 4.0
CONSTANT_GAIN = KAPPA * (2.0 + COARSE * COARSE_SCALE)
LANES = 128


def rolled(x, shift, axis):
    size = x.shape[axis]
    return pltpu.roll(x, shift % size, axis)


def rolled_z(x, shift):
    rows, subs, nz = x.shape
    return rolled(x.reshape(rows * subs, nz), shift, 1).reshape(x.shape)


def fill_ends(ref, plane, nj):
    ref[plane, 0] = rolled(ref[plane, nj], 1, 0)
    ref[plane, nj + 1] = rolled(ref[plane, 1], -1, 0)


def across(ref, plane, start, rows):
    wide = ref[plane, pl.ds(start, rows + 2)]
    center = wide[1 : rows + 1]
    beside = wide[:rows] + wide[2:] + rolled_z(center, 1) + rolled_z(center, -1)
    return center, beside


def dot_exact(x, table):
    high = x.astype(jnp.bfloat16)
    rest = x - high.astype(jnp.float32)
    middle = rest.astype(jnp.bfloat16)
    low = (rest - middle.astype(jnp.float32)).astype(jnp.bfloat16)
    dot = functools.partial(jnp.dot, preferred_element_type=jnp.float32)
    return dot(high, table) + dot(middle, table) + dot(low, table)


def pair_up(sums_ref, plane, table_ref, out_ref, scale=1.0):
    nc, _, nz = sums_ref.shape[1:]
    step = min(nc, 8)

    def body(i):
        at = i * step
        block = sums_ref[plane, pl.ds(at, step)].reshape(step * 8, nz)
        out = dot_exact(block, table_ref[...]) * scale
        out_ref[pl.ds(at, step)] = out.reshape(step, 8, nz // 2)

    lax.fori_loop(0, nc // step, lambda i, c: (body(i), c)[1], 0)


def loop(count, body, unroll=2):
    lax.fori_loop(0, count, lambda i, c: (body(i), c)[1], 0, unroll=min(unroll, count))


def convert(plane, x, k, X, D, T, nj):
    tiles = T.shape[0]

    def split(i):
        rows = pl.ds(pl.multiple_of(i * 16, 16), 16)
        for t in range(tiles):
            T[t, rows, :] = plane[x, rows, pl.ds(t * LANES, LANES)]

    loop(nj // 2, split, 4)

    def body(j):
        rows = pl.ds(j, 8, stride=nj)
        row = jnp.concatenate([T[t, rows, :] for t in range(tiles)], axis=1)
        X[k, j + 1] = row
        D[k, j + 1] = rolled(row, -1, 1) - rolled(row, 1, 1)

    loop(nj, body, 16)
    fill_ends(X, k, nj)


def prepare_kernel(own, X, D, curved, rest, T):
    nj = X.shape[1] - 2
    for x in range(2):
        convert(own, x, x, X, D, T, nj)
        fill_ends(D, x, nj)

        def body(i, x=x):
            j = 2 * i
            center, beside = X[x, pl.ds(j, 4)], D[x, pl.ds(j, 4)]
            middle = center[1:3]
            double = 2.0 * middle
            curve_yy = center[2:] + center[:2] - double
            curve_zz = rolled_z(middle, 1) + rolled_z(middle, -1) - double
            cross_yz = beside[2:] - beside[:2]
            curved[x, pl.ds(j, 2)] = curve_yy + curve_zz
            rest[x, pl.ds(j, 2)] = 0.0625 * (cross_yz * cross_yz) - curve_yy * curve_zz

        loop(nj // 2, body, 8)


def source_kernel(
    X, D, curved, rest, left, right, table, f00, f01, f10, f11, s0, s1, total, XH, DH, G, T, acc
):
    nj = X.shape[1] - 2
    half = nj // 2
    outs = ((f00, f01), (f10, f11))
    convert(left, 0, 0, XH, DH, T, nj)
    convert(right, 0, 1, XH, DH, T, nj)
    lowers = ((XH, DH, 0), (X, D, 0))
    uppers = ((X, D, 1), (XH, DH, 1))
    acc[...] = jnp.zeros_like(acc)
    for x in range(2):
        for h in range(2):
            def cells(i, x=x, h=h):
                j = h * half + 2 * i
                (lower, lower_d, l), (upper, upper_d, u) = lowers[x], uppers[x]
                above, below = upper[u, pl.ds(j, 4)], lower[l, pl.ds(j, 4)]
                tilt = above - below
                curve_xx = above[1:3] + below[1:3] - 2.0 * X[x, pl.ds(j + 1, 2)]
                cross_xy = tilt[2:] - tilt[:2]
                cross_xz = upper_d[u, pl.ds(j + 1, 2)] - lower_d[l, pl.ds(j + 1, 2)]
                forcing = rest[x, pl.ds(j, 2)] + 0.0625 * (cross_xy * cross_xy + cross_xz * cross_xz)
                forcing = forcing - curve_xx * curved[x, pl.ds(j, 2)]
                outs[x][h][pl.ds(2 * i, 2)] = forcing
                pair = forcing[0] + forcing[1]
                G[x, h * (half // 2) + i] = pair
                acc[...] += pair

            loop(half // 2, cells, 4)
    folded = acc[...]
    width = folded.shape[1]
    total[...] = sum(folded[:, k : k + LANES] for k in range(0, width, LANES))
    pair_up(G, 0, table, s0)
    pair_up(G, 1, table, s1)


def load_rows(refs, V, nj):
    half = nj // 2
    for h in range(2):
        def body(i, h=h):
            V[0, h * half + i + 1] = refs[0][h][i] + refs[1][h][i]

        loop(half, body, 8)
    fill_ends(V, 0, nj)


def rhs_first_kernel(f00, f01, f10, f11, table, out, V, G):
    nj = V.shape[1] - 2
    load_rows(((f00, f01), (f10, f11)), V, nj)

    def body(i):
        center, beside = across(V, 0, 2 * i, 2)
        value = (1.0 - 5.0 * KAPPA) * center + KAPPA * beside
        G[0, i] = value[0] + value[1]

    loop(nj // 2, body, 8)
    pair_up(G, 0, table, out, 0.125)


def rhs_later_kernel(f00, f01, f10, f11, v00, v01, v10, v11, table, out, V, G):
    nj = V.shape[1] - 2
    half = nj // 2
    load_rows(((v00, v01), (v10, v11)), V, nj)
    for h in range(2):
        def body(i, h=h):
            center, beside = across(V, 0, h * half + 2 * i, 2)
            forcing = (f00, f01)[h][pl.ds(2 * i, 2)] + (f10, f11)[h][pl.ds(2 * i, 2)]
            value = forcing - (5.0 * center - beside)
            G[0, h * (half // 2) + i] = value[0] + value[1]

        loop(half // 2, body, 8)
    pair_up(G, 0, table, out, 0.125)


def correct(corrections, table, C):
    nc, _, nz = C.shape[1:]
    step = min(nc, 8)
    for k in range(3):
        def body(i, k=k):
            at = i * step
            block = corrections[k][pl.ds(at, step)].reshape(step * 8, nz // 2)
            C[k, pl.ds(at, step)] = dot_exact(block, table[...]).reshape(step, 8, nz)

        loop(nc // step, body, 1)


def smoothed(W, V, force, nj):
    half = nj // 2
    for k in range(4):
        for h in range(2):
            def body(i, k=k, h=h):
                j = h * half + 2 * i
                center, beside = across(W, k + 1, j, 2)
                beside = beside + W[k, pl.ds(j + 1, 2)] + W[k + 2, pl.ds(j + 1, 2)]
                value = (1.0 - 6.0 * KAPPA) * center + KAPPA * (force[k][h][pl.ds(2 * i, 2)] + beside)
                V[k, pl.ds(j + 1, 2)] = value

            loop(half // 2, body, 8)
        fill_ends(V, k, nj)


def residual_rows(V, x, h, i, force, half):
    j = h * half + 2 * i
    center, beside = across(V, x + 1, j, 2)
    beside = beside + V[x, pl.ds(j + 1, 2)] + V[x + 2, pl.ds(j + 1, 2)]
    return center, force[x + 1][h][pl.ds(2 * i, 2)] - (6.0 * center - beside)


def fold_row(value):
    return jnp.sum(jnp.sum(value, axis=0, keepdims=True), axis=1, keepdims=True)


def stats_row(rest, *figures):
    lane = lax.broadcasted_iota(jnp.int32, (1, LANES), 1)
    for at, figure in enumerate(figures):
        rest = jnp.where(lane == at, figure, rest)
    return rest


def halves(refs):
    return tuple((refs[2 * k], refs[2 * k + 1]) for k in range(len(refs) // 2))


def middle_kernel(*refs):
    (left, own, right), rest = tuple(halves(refs[4 * k : 4 * k + 4]) for k in range(3)), refs[12:]
    c_own, c_left, c_right, shift, table, pairs, v00, v01, v10, v11, s0, s1, stats, W, V, C, G, acc = rest
    nj = W.shape[1] - 2
    half = nj // 2
    outs = ((v00, v01), (v10, v11))
    force = left + own + right
    correct((c_left, c_own, c_right), table, C)
    for k in range(6):
        for h in range(2):
            def body(i, k=k, h=h):
                extra = C[k // 2, h * (half // 2) + i]
                value = KAPPA * force[k][h][pl.ds(2 * i, 2)]
                W[k, pl.ds(h * half + 2 * i + 1, 2)] = value + extra[None]

            loop(half // 2, body, 8)
        if 1 <= k <= 4:
            fill_ends(W, k, nj)
    smoothed(W, V, force[1:5], nj)
    acc[...] = jnp.zeros_like(acc)
    for x in range(2):
        for h in range(2):
            def body(i, x=x, h=h):
                center, residue = residual_rows(V, x, h, i, force[1:5], half)
                value = center + KAPPA * residue
                outs[x][h][pl.ds(2 * i, 2)] = value
                G[x, h * (half // 2) + i] = value[0] + value[1]
                offset = residue - shift[...][None]
                acc[0] += offset[0] + offset[1]
                acc[1] += offset[0] * offset[0] + offset[1] * offset[1]

            loop(half // 2, body, 8)
    zero = jnp.zeros((1, LANES), jnp.float32)
    stats[...] = stats_row(zero, zero, zero, zero, fold_row(acc[0]), fold_row(acc[1]))
    pair_up(G, 0, pairs, s0)
    pair_up(G, 1, pairs, s1)


def last_kernel(*refs):
    f_left, f_right = halves(refs[0:2]), halves(refs[2:4])
    f_own = halves(refs[4:8])
    v_left, v_own, v_right = (halves(refs[4 * k + 8 : 4 * k + 12]) for k in range(3))
    c_own, c_left, c_right, shift, total, first, table, out, stats, W, V, C, acc = refs[20:]
    nj = W.shape[1] - 2
    half = nj // 2
    force = f_left + f_own + f_right
    start = v_left + v_own + v_right
    correct((c_left, c_own, c_right), table, C)
    for k in range(6):
        for h in range(2):
            def body(i, k=k, h=h):
                extra = C[k // 2, h * (half // 2) + i]
                W[k, pl.ds(h * half + 2 * i + 1, 2)] = start[k][h][pl.ds(2 * i, 2)] + extra[None]

            loop(half // 2, body, 8)
        if 1 <= k <= 4:
            fill_ends(W, k, nj)
    smoothed(W, V, force, nj)
    acc[...] = jnp.zeros_like(acc)
    for x in range(2):
        for h in range(2):
            def body(i, x=x, h=h):
                center, residue = residual_rows(V, x, h, i, force, half)
                out[x, pl.ds(h * half + 2 * i, 2)] = center
                offset = residue - shift[...][None]
                acc[0] += offset[0] + offset[1]
                acc[1] += offset[0] * offset[0] + offset[1] * offset[1]

            loop(half // 2, body, 8)
    stats[...] = stats_row(first[...], fold_row(total[...]), fold_row(acc[0]), fold_row(acc[1]))


def natural_kernel(field, out, T):
    nj = field.shape[1]
    tiles = T.shape[0]
    for x in range(2):
        def body(j, x=x):
            row = field[x, j]
            for t in range(tiles):
                T[t, pl.ds(j, 8, stride=nj), :] = row[:, t * LANES : (t + 1) * LANES]

        loop(nj, body, 8)

        def join(i, x=x):
            rows = pl.ds(pl.multiple_of(i * 16, 16), 16)
            for t in range(tiles):
                out[x, rows, pl.ds(t * LANES, LANES)] = T[t, rows, :]

        loop(nj // 2, join, 4)


def finish_kernel(share, figures, field, out, norms):
    devices = figures.shape[0]
    sums = figures[:, 0:1]
    mean = -jnp.sum(sums, axis=0, keepdims=True) / (share * devices)
    off = mean + sums / share
    for c, at in enumerate((3, 1)):
        linear, square = figures[:, at : at + 1], figures[:, at + 1 : at + 2]
        squares = square + 2.0 * off * linear + share * off * off
        total = jnp.sum(squares, axis=0, keepdims=True) / (share * devices)
        norms[c] = jnp.sqrt(total)[0, 0]
    gain = mean * (CONSTANT_GAIN * CYCLES)
    for x in range(2):
        def body(i, x=x):
            rows = pl.ds(pl.multiple_of(i * 16, 16), 16)
            out[x, rows, :] = field[x, rows, :] + gain

        loop(field.shape[1] // 16, body, 4)


VMEM = pl.BlockSpec(memory_space=pltpu.VMEM)
SMEM = pl.BlockSpec(memory_space=pltpu.SMEM)


def call(kernel, args, outs, scratch, flops, out_specs=None):
    moved = 4 * (sum(a.size for a in args) + sum(int(np.prod(o)) for o in outs))
    return pl.pallas_call(
        kernel,
        out_shape=[jax.ShapeDtypeStruct(o, jnp.float32) for o in outs],
        in_specs=[VMEM] * len(args),
        out_specs=out_specs or [VMEM] * len(outs),
        scratch_shapes=[pltpu.VMEM(s, jnp.float32) for s in scratch],
        compiler_params=pltpu.CompilerParams(vmem_limit_bytes=24 * 2**20),
        cost_estimate=pl.CostEstimate(flops=flops, bytes_accessed=moved, transcendentals=0),
    )(*args)


def from_left(x):
    count = lax.axis_size("gx")
    return lax.ppermute(x, "gx", [(i, (i + 1) % count) for i in range(count)])


def from_right(x):
    count = lax.axis_size("gx")
    return lax.ppermute(x, "gx", [((i + 1) % count, i) for i in range(count)])


def gathered(row):
    count = lax.axis_size("gx")
    spread = jnp.broadcast_to(row, (count, *row.shape[1:]))
    return lax.all_to_all(spread, "gx", 0, 0, tiled=True)


def coarse_beside(field):
    first, last = field[:1], field[-1:]
    below = jnp.concatenate([jnp.roll(last, 1, 1), field[:-1]], 0)
    above = jnp.concatenate([field[1:], jnp.roll(first, -1, 1)], 0)
    return below + above + jnp.roll(field, 1, 2) + jnp.roll(field, -1, 2)


def both(to_right, to_left):
    left = from_left(to_right)
    right = from_right(to_left)
    return left, right


def coarse_part(local, s0, s1, weight, chunks):
    moved = []
    left, right = both(s1, s0)
    moved.append(both(chunks[0], chunks[0]))
    rhs = local + (weight * 0.125) * (left + right)
    step = RELAX * COARSE_SCALE / 6.0
    field = step * rhs
    for sweep in range(1, COARSE):
        left, right = both(field, field)
        moved.append(both(chunks[sweep], chunks[sweep]))
        part = (1.0 - RELAX) * field + step * rhs + KAPPA * coarse_beside(field)
        field = part + KAPPA * (left + right)
    left, right = both(field, field)
    lefts, rights = zip(*moved)
    return (field, left, right), lefts, rights


def whole(potential):
    _, ny, nz = potential.shape
    nj, nc = ny // 8, ny // 16
    width = nz // 2
    share = float(potential.size)
    columns = np.arange(nz)[:, None] // 2 == np.arange(width)[None, :]
    pairs = jnp.asarray(columns, jnp.bfloat16)
    copies = jnp.asarray(columns.T, jnp.bfloat16)
    chunk = (nj // 2, 8, nz)
    coarse = (nc, 8, width)
    tall = (nj + 2, 8, nz)

    left = from_left(potential[1:])
    right = from_right(potential[:1])
    tiles = (nz // LANES, ny, LANES)
    prepared = call(
        prepare_kernel, (potential,), [(2, *tall), (2, *tall), (2, nj, 8, nz), (2, nj, 8, nz)], [tiles], 10**8
    )
    *forcing, s0, s1, total = call(
        source_kernel, (*prepared, left, right, pairs), [chunk] * 4 + [coarse] * 2 + [(8, LANES)],
        [(2, *tall), (2, *tall), (2, nc, 8, nz), tiles, (8, nz)], 10**8,
    )
    shift = jnp.broadcast_to(jnp.sum(total) / share, (8, nz))
    (local,) = call(
        rhs_first_kernel, (*forcing, pairs), [coarse], [(1, *tall), (1, nc, 8, nz)], 3 * 10**7
    )
    correction, f_left, f_right = coarse_part(local, s0, s1, KAPPA, forcing)
    scratch = [(6, *tall), (4, *tall), (3, nc, 8, nz)]
    *field, s0, s1, first = call(
        middle_kernel, (*f_left, *forcing, *f_right, *correction, shift, copies, pairs),
        [chunk] * 4 + [coarse] * 2 + [(1, LANES)], [*scratch, (2, nc, 8, nz), (2, 8, nz)], 10**8,
    )
    (local,) = call(
        rhs_later_kernel, (*forcing, *field, pairs), [coarse], [(1, *tall), (1, nc, 8, nz)], 3 * 10**7
    )
    correction, v_left, v_right = coarse_part(local, s0, s1, 1.0, field)
    result, last = call(
        last_kernel,
        (*f_left[2:], *f_right[:2], *forcing, *v_left, *field, *v_right, *correction, shift, total, first, copies),
        [(2, nj, 8, nz), (1, LANES)], [*scratch, (2, 8, nz)], 10**8,
    )
    (result,) = call(natural_kernel, (result,), [potential.shape], [tiles], 3 * 10**7)
    result, norms = call(
        functools.partial(finish_kernel, share), (gathered(last), result),
        [potential.shape, (CYCLES,)], [], 10**7, [VMEM, SMEM],
    )
    return (result, norms)


def solution(mesh):
    in_specs = (P(("runs", "gx"), None, None),)
    out_specs = (P(("runs", "gx"), None, None), P("runs"))
    return jax.shard_map(whole, mesh=mesh, in_specs=in_specs, out_specs=out_specs, check_vma=False)
```

```python
import functools

import jax
import jax.numpy as jnp
import numpy as np
from jax import lax
from jax.experimental import pallas as pl
from jax.experimental.pallas import tpu as pltpu
from jax.sharding import PartitionSpec as P

CYCLES = 2
COARSE = 4
RELAX = 0.8
KAPPA = RELAX / 6.0
COARSE_SCALE = 4.0
CONSTANT_GAIN = KAPPA * (2.0 + COARSE * COARSE_SCALE)
LANES = 128


def rolled(x, shift, axis):
    size = x.shape[axis]
    return pltpu.roll(x, shift % size, axis)


def rolled_z(x, shift):
    rows, subs, nz = x.shape
    return rolled(x.reshape(rows * subs, nz), shift, 1).reshape(x.shape)


def fill_ends(ref, plane, nj):
    ref[plane, 0] = rolled(ref[plane, nj], 1, 0)
    ref[plane, nj + 1] = rolled(ref[plane, 1], -1, 0)


def across(ref, plane, start, rows):
    wide = ref[plane, pl.ds(start, rows + 2)]
    center = wide[1 : rows + 1]
    beside = wide[:rows] + wide[2:] + rolled_z(center, 1) + rolled_z(center, -1)
    return center, beside


def dot_exact(x, table, side=0):
    high = x.astype(jnp.bfloat16)
    rest = x - high.astype(jnp.float32)
    middle = rest.astype(jnp.bfloat16)
    low = (rest - middle.astype(jnp.float32)).astype(jnp.bfloat16)
    parts = jnp.concatenate([high, middle, low], 0)
    out = lax.dot_general(parts, table, (((1,), (side,)), ((), ())), preferred_element_type=jnp.float32)
    rows = x.shape[0]
    return out[:rows] + out[rows : 2 * rows] + out[2 * rows :]


def pair_up(sums_ref, plane, table_ref, out_ref, scale=1.0):
    nc, _, nz = sums_ref.shape[1:]
    step = min(nc, 32)

    def body(i):
        at = i * step
        block = sums_ref[plane, pl.ds(at, step)].reshape(step * 8, nz)
        out = dot_exact(block, table_ref[...]) * scale
        out_ref[pl.ds(at, step)] = out.reshape(step, 8, nz // 2)

    lax.fori_loop(0, nc // step, lambda i, c: (body(i), c)[1], 0)


def loop(count, body, unroll=2):
    lax.fori_loop(0, count, lambda i, c: (body(i), c)[1], 0, unroll=min(unroll, count))


def convert(plane, x, k, X, D, T, nj):
    tiles = T.shape[0]

    def split(i):
        rows = pl.ds(pl.multiple_of(i * 16, 16), 16)
        for t in range(tiles):
            T[t, rows, :] = plane[x, rows, pl.ds(t * LANES, LANES)]

    loop(nj // 2, split, 4)

    def body(j):
        rows = pl.ds(j, 8, stride=nj)
        row = jnp.concatenate([T[t, rows, :] for t in range(tiles)], axis=1)
        X[k, j + 1] = row
        D[k, j + 1] = rolled(row, -1, 1) - rolled(row, 1, 1)

    loop(nj, body, 16)
    fill_ends(X, k, nj)


def prepare_kernel(own, X, D, curved, rest, T):
    nj = X.shape[1] - 2
    for x in range(2):
        convert(own, x, x, X, D, T, nj)
        fill_ends(D, x, nj)

        def body(i, x=x):
            j = 2 * i
            center, beside = X[x, pl.ds(j, 4)], D[x, pl.ds(j, 4)]
            middle = center[1:3]
            double = 2.0 * middle
            curve_yy = center[2:] + center[:2] - double
            curve_zz = rolled_z(middle, 1) + rolled_z(middle, -1) - double
            cross_yz = beside[2:] - beside[:2]
            curved[x, pl.ds(j, 2)] = curve_yy + curve_zz
            rest[x, pl.ds(j, 2)] = 0.0625 * (cross_yz * cross_yz) - curve_yy * curve_zz

        loop(nj // 2, body, 8)


def source_kernel(
    X, D, curved, rest, left, right, table, f00, f01, f10, f11, s0, s1, total, XH, DH, G, T, acc
):
    nj = X.shape[1] - 2
    half = nj // 2
    outs = ((f00, f01), (f10, f11))
    convert(left, 0, 0, XH, DH, T, nj)
    convert(right, 0, 1, XH, DH, T, nj)
    lowers = ((XH, DH, 0), (X, D, 0))
    uppers = ((X, D, 1), (XH, DH, 1))
    acc[...] = jnp.zeros_like(acc)
    for x in range(2):
        for h in range(2):
            def cells(i, x=x, h=h):
                j = h * half + 2 * i
                (lower, lower_d, l), (upper, upper_d, u) = lowers[x], uppers[x]
                above, below = upper[u, pl.ds(j, 4)], lower[l, pl.ds(j, 4)]
                tilt = above - below
                curve_xx = above[1:3] + below[1:3] - 2.0 * X[x, pl.ds(j + 1, 2)]
                cross_xy = tilt[2:] - tilt[:2]
                cross_xz = upper_d[u, pl.ds(j + 1, 2)] - lower_d[l, pl.ds(j + 1, 2)]
                forcing = rest[x, pl.ds(j, 2)] + 0.0625 * (cross_xy * cross_xy + cross_xz * cross_xz)
                forcing = forcing - curve_xx * curved[x, pl.ds(j, 2)]
                outs[x][h][pl.ds(2 * i, 2)] = forcing
                pair = forcing[0] + forcing[1]
                G[x, h * (half // 2) + i] = pair
                acc[...] += pair

            loop(half // 2, cells, 4)
    folded = acc[...]
    width = folded.shape[1]
    total[...] = sum(folded[:, k : k + LANES] for k in range(0, width, LANES))
    pair_up(G, 0, table, s0)
    pair_up(G, 1, table, s1)


def load_rows(refs, V, nj):
    half = nj // 2
    for h in range(2):
        def body(i, h=h):
            V[0, h * half + i + 1] = refs[0][h][i] + refs[1][h][i]

        loop(half, body, 8)
    fill_ends(V, 0, nj)


def rhs_first_kernel(f00, f01, f10, f11, table, out, V, G):
    nj = V.shape[1] - 2
    load_rows(((f00, f01), (f10, f11)), V, nj)

    def body(i):
        center, beside = across(V, 0, 2 * i, 2)
        value = (1.0 - 5.0 * KAPPA) * center + KAPPA * beside
        G[0, i] = value[0] + value[1]

    loop(nj // 2, body, 8)
    pair_up(G, 0, table, out, 0.125)


def rhs_later_kernel(f00, f01, f10, f11, v00, v01, v10, v11, table, out, V, G):
    nj = V.shape[1] - 2
    half = nj // 2
    load_rows(((v00, v01), (v10, v11)), V, nj)
    for h in range(2):
        def body(i, h=h):
            center, beside = across(V, 0, h * half + 2 * i, 2)
            forcing = (f00, f01)[h][pl.ds(2 * i, 2)] + (f10, f11)[h][pl.ds(2 * i, 2)]
            value = forcing - (5.0 * center - beside)
            G[0, h * (half // 2) + i] = value[0] + value[1]

        loop(half // 2, body, 8)
    pair_up(G, 0, table, out, 0.125)


def correct(corrections, table, C):
    nc, _, nz = C.shape[1:]
    step = min(nc, 32)
    for k in range(3):
        def body(i, k=k):
            at = i * step
            block = corrections[k][pl.ds(at, step)].reshape(step * 8, nz // 2)
            C[k, pl.ds(at, step)] = dot_exact(block, table[...], 1).reshape(step, 8, nz)

        loop(nc // step, body, 1)


def spread_planes(start, weight, force, C, W, U, nj):
    half = nj // 2
    for k in range(6):
        for h in range(2):
            def body(i, k=k, h=h):
                extra = C[k // 2, h * (half // 2) + i]
                at = pl.ds(h * half + 2 * i + 1, 2)
                W[k, at] = weight * start[k][h][pl.ds(2 * i, 2)] + extra[None]
                if 1 <= k <= 4:
                    U[k - 1, at] = KAPPA * force[k - 1][h][pl.ds(2 * i, 2)]

            loop(half // 2, body, 4)
        if 1 <= k <= 4:
            fill_ends(W, k, nj)


def smoothed(W, V, U, nj):
    def plane(k):
        def body(i):
            j = 2 * i
            center, beside = across(W, k + 1, j, 2)
            at = pl.ds(j + 1, 2)
            beside = beside + W[k, at] + W[k + 2, at]
            V[k, at] = (1.0 - 6.0 * KAPPA) * center + U[k, at] + KAPPA * beside

        loop(nj // 2, body, 8)
        fill_ends(V, k, nj)

    loop(4, plane, 1)


def residual_rows(V, U, x, j):
    center, beside = across(V, x + 1, j, 2)
    at = pl.ds(j + 1, 2)
    beside = beside + V[x, at] + V[x + 2, at]
    return center, (1.0 / KAPPA) * U[x + 1, at] - (6.0 * center - beside)


def fold_row(value):
    return jnp.sum(jnp.sum(value, axis=0, keepdims=True), axis=1, keepdims=True)


def stats_row(rest, *figures):
    lane = lax.broadcasted_iota(jnp.int32, (1, LANES), 1)
    for at, figure in enumerate(figures):
        rest = jnp.where(lane == at, figure, rest)
    return rest


def halves(refs):
    return tuple((refs[2 * k], refs[2 * k + 1]) for k in range(len(refs) // 2))


def add_figures(acc, residue, shift):
    offset = residue - shift[...][None]
    acc[0] += offset[0] + offset[1]
    acc[1] += offset[0] * offset[0] + offset[1] * offset[1]


def middle_kernel(*refs):
    (left, own, right), rest = tuple(halves(refs[4 * k : 4 * k + 4]) for k in range(3)), refs[12:]
    c_own, c_left, c_right, shift, table, v00, v01, v10, v11, s0, s1, stats, W, V, U, C, G, acc = rest
    nj = W.shape[1] - 2
    half = nj // 2
    outs = ((v00, v01), (v10, v11))
    force = left + own + right
    correct((c_left, c_own, c_right), table, C)
    spread_planes(force, KAPPA, force[1:5], C, W, U, nj)
    smoothed(W, V, U, nj)
    acc[...] = jnp.zeros_like(acc)
    for x in range(2):
        for h in range(2):
            def body(i, x=x, h=h):
                center, residue = residual_rows(V, U, x, h * half + 2 * i)
                value = center + KAPPA * residue
                outs[x][h][pl.ds(2 * i, 2)] = value
                G[x, h * (half // 2) + i] = value[0] + value[1]
                add_figures(acc, residue, shift)

            loop(half // 2, body, 4)
    zero = jnp.zeros((1, LANES), jnp.float32)
    stats[...] = stats_row(zero, zero, zero, zero, fold_row(acc[0]), fold_row(acc[1]))
    pair_up(G, 0, table, s0)
    pair_up(G, 1, table, s1)


def last_kernel(*refs):
    f_left, f_right = halves(refs[0:2]), halves(refs[2:4])
    f_own = halves(refs[4:8])
    v_left, v_own, v_right = (halves(refs[4 * k + 8 : 4 * k + 12]) for k in range(3))
    c_own, c_left, c_right, shift, total, first, table, out, stats, W, V, U, C, acc = refs[20:]
    nj = W.shape[1] - 2
    correct((c_left, c_own, c_right), table, C)
    spread_planes(v_left + v_own + v_right, 1.0, f_left + f_own + f_right, C, W, U, nj)
    smoothed(W, V, U, nj)
    acc[...] = jnp.zeros_like(acc)

    def plane(x):
        def body(i):
            center, residue = residual_rows(V, U, x, 2 * i)
            out[x, pl.ds(2 * i, 2)] = center
            add_figures(acc, residue, shift)

        loop(nj // 2, body, 8)

    loop(2, plane, 1)
    row = stats_row(first[...], fold_row(total[...]), fold_row(acc[0]), fold_row(acc[1]))
    stats[...] = jnp.broadcast_to(row[None], stats.shape)


def natural_kernel(field, out, T):
    nj = field.shape[1]
    tiles = T.shape[0]
    for x in range(2):
        def body(j, x=x):
            row = field[x, j]
            for t in range(tiles):
                T[t, pl.ds(j, 8, stride=nj), :] = row[:, t * LANES : (t + 1) * LANES]

        loop(nj, body, 8)

        def join(i, x=x):
            rows = pl.ds(pl.multiple_of(i * 16, 16), 16)
            for t in range(tiles):
                out[x, rows, pl.ds(t * LANES, LANES)] = T[t, rows, :]

        loop(nj // 2, join, 4)


def finish_kernel(share, figures, field, out, norms):
    devices = figures.shape[0]
    sums = figures[:, 0:1]
    mean = -jnp.sum(sums, axis=0, keepdims=True) / (share * devices)
    off = mean + sums / share
    for c, at in enumerate((3, 1)):
        linear, square = figures[:, at : at + 1], figures[:, at + 1 : at + 2]
        squares = square + 2.0 * off * linear + share * off * off
        total = jnp.sum(squares, axis=0, keepdims=True) / (share * devices)
        norms[c] = jnp.sqrt(total)[0, 0]
    gain = mean * (CONSTANT_GAIN * CYCLES)
    for x in range(2):
        def body(i, x=x):
            rows = pl.ds(pl.multiple_of(i * 16, 16), 16)
            out[x, rows, :] = field[x, rows, :] + gain

        loop(field.shape[1] // 16, body, 4)


VMEM = pl.BlockSpec(memory_space=pltpu.VMEM)
SMEM = pl.BlockSpec(memory_space=pltpu.SMEM)


def call(kernel, args, outs, scratch, flops, out_specs=None):
    moved = 4 * (sum(a.size for a in args) + sum(int(np.prod(o)) for o in outs))
    return pl.pallas_call(
        kernel,
        out_shape=[jax.ShapeDtypeStruct(o, jnp.float32) for o in outs],
        in_specs=[VMEM] * len(args),
        out_specs=out_specs or [VMEM] * len(outs),
        scratch_shapes=[pltpu.VMEM(s, jnp.float32) for s in scratch],
        compiler_params=pltpu.CompilerParams(vmem_limit_bytes=24 * 2**20),
        cost_estimate=pl.CostEstimate(flops=flops, bytes_accessed=moved, transcendentals=0),
    )(*args)


def from_left(x):
    count = lax.axis_size("gx")
    return lax.ppermute(x, "gx", [(i, (i + 1) % count) for i in range(count)])


def from_right(x):
    count = lax.axis_size("gx")
    return lax.ppermute(x, "gx", [((i + 1) % count, i) for i in range(count)])


def gathered(rows):
    return lax.all_to_all(rows, "gx", 0, 0, tiled=True)


def coarse_beside(field):
    first, last = field[:1], field[-1:]
    below = jnp.concatenate([jnp.roll(last, 1, 1), field[:-1]], 0)
    above = jnp.concatenate([field[1:], jnp.roll(first, -1, 1)], 0)
    return below + above + jnp.roll(field, 1, 2) + jnp.roll(field, -1, 2)


def both(to_right, to_left):
    left = from_left(to_right)
    right = from_right(to_left)
    return left, right


def coarse_part(local, s0, s1, weight, chunks):
    moved = []
    left, right = both(s1, s0)
    moved.append(both(chunks[0], chunks[0]))
    rhs = local + (weight * 0.125) * (left + right)
    step = RELAX * COARSE_SCALE / 6.0
    field = step * rhs
    for sweep in range(1, COARSE):
        left, right = both(field, field)
        moved.append(both(chunks[sweep], chunks[sweep]))
        part = (1.0 - RELAX) * field + step * rhs + KAPPA * coarse_beside(field)
        field = part + KAPPA * (left + right)
    left, right = both(field, field)
    lefts, rights = zip(*moved)
    return (field, left, right), lefts, rights


def whole(potential):
    _, ny, nz = potential.shape
    nj, nc = ny // 8, ny // 16
    width = nz // 2
    share = float(potential.size)
    columns = np.arange(nz)[:, None] // 2 == np.arange(width)[None, :]
    pairs = jnp.asarray(columns, jnp.bfloat16)
    chunk = (nj // 2, 8, nz)
    coarse = (nc, 8, width)
    tall = (nj + 2, 8, nz)

    tail, potential = lax.optimization_barrier((potential[1:], potential))
    left = from_left(tail)
    right = from_right(potential[:1])
    tiles = (nz // LANES, ny, LANES)
    prepared = call(
        prepare_kernel, (potential,), [(2, *tall), (2, *tall), (2, nj, 8, nz), (2, nj, 8, nz)], [tiles], 10**8
    )
    *forcing, s0, s1, total = call(
        source_kernel, (*prepared, left, right, pairs), [chunk] * 4 + [coarse] * 2 + [(8, LANES)],
        [(2, *tall), (2, *tall), (2, nc, 8, nz), tiles, (8, nz)], 10**8,
    )
    shift = jnp.broadcast_to(jnp.sum(total) / share, (8, nz))
    (local,) = call(
        rhs_first_kernel, (*forcing, pairs), [coarse], [(1, *tall), (1, nc, 8, nz)], 3 * 10**7
    )
    correction, f_left, f_right = coarse_part(local, s0, s1, KAPPA, forcing)
    scratch = [(6, *tall), (4, *tall), (4, *tall), (3, nc, 8, nz)]
    *field, s0, s1, first = call(
        middle_kernel, (*f_left, *forcing, *f_right, *correction, shift, pairs),
        [chunk] * 4 + [coarse] * 2 + [(1, LANES)], [*scratch, (2, nc, 8, nz), (2, 8, nz)], 10**8,
    )
    (local,) = call(
        rhs_later_kernel, (*forcing, *field, pairs), [coarse], [(1, *tall), (1, nc, 8, nz)], 3 * 10**7
    )
    correction, v_left, v_right = coarse_part(local, s0, s1, 1.0, field)
    result, last = call(
        last_kernel,
        (*f_left[2:], *f_right[:2], *forcing, *v_left, *field, *v_right, *correction, shift, total, first, pairs),
        [(2, nj, 8, nz), (lax.axis_size("gx"), 1, LANES)], [*scratch, (2, 8, nz)], 10**8,
    )
    (result,) = call(natural_kernel, (result,), [potential.shape], [tiles], 3 * 10**7)
    result, norms = call(
        functools.partial(finish_kernel, share), (gathered(last).reshape(-1, LANES), result),
        [potential.shape, (CYCLES,)], [], 10**7, [VMEM, SMEM],
    )
    return (result, norms)


def solution(mesh):
    in_specs = (P(("runs", "gx"), None, None),)
    out_specs = (P(("runs", "gx"), None, None), P("runs"))
    return jax.shard_map(whole, mesh=mesh, in_specs=in_specs, out_specs=out_specs, check_vma=False)
```

```python
import functools

import jax
import jax.numpy as jnp
import numpy as np
from jax import lax
from jax.experimental import pallas as pl
from jax.experimental.pallas import tpu as pltpu
from jax.sharding import PartitionSpec as P

CYCLES = 2
COARSE = 4
RELAX = 0.8
KAPPA = RELAX / 6.0
COARSE_SCALE = 4.0
CONSTANT_GAIN = KAPPA * (2.0 + COARSE * COARSE_SCALE)
LANES = 128


def rolled(x, shift, axis):
    size = x.shape[axis]
    return pltpu.roll(x, shift % size, axis)


def rolled_z(x, shift):
    rows, subs, nz = x.shape
    return rolled(x.reshape(rows * subs, nz), shift, 1).reshape(x.shape)


def fill_ends(ref, plane, nj):
    ref[plane, 0] = rolled(ref[plane, nj], 1, 0)
    ref[plane, nj + 1] = rolled(ref[plane, 1], -1, 0)


def across(ref, plane, start, rows):
    wide = ref[plane, pl.ds(start, rows + 2)]
    center = wide[1 : rows + 1]
    beside = wide[:rows] + wide[2:] + rolled_z(center, 1) + rolled_z(center, -1)
    return center, beside


def dot_exact(x, table, side=0):
    high = x.astype(jnp.bfloat16)
    rest = x - high.astype(jnp.float32)
    middle = rest.astype(jnp.bfloat16)
    low = (rest - middle.astype(jnp.float32)).astype(jnp.bfloat16)
    parts = jnp.concatenate([high, middle, low], 0)
    out = lax.dot_general(parts, table, (((1,), (side,)), ((), ())), preferred_element_type=jnp.float32)
    rows = x.shape[0]
    return out[:rows] + out[rows : 2 * rows] + out[2 * rows :]


def pair_up(sums_ref, plane, table_ref, out_ref, scale=1.0):
    nc, _, nz = sums_ref.shape[1:]
    step = min(nc, 32)

    def body(i):
        at = i * step
        block = sums_ref[plane, pl.ds(at, step)].reshape(step * 8, nz)
        out = dot_exact(block, table_ref[...]) * scale
        out_ref[pl.ds(at, step)] = out.reshape(step, 8, nz // 2)

    lax.fori_loop(0, nc // step, lambda i, c: (body(i), c)[1], 0)


def loop(count, body, unroll=2):
    lax.fori_loop(0, count, lambda i, c: (body(i), c)[1], 0, unroll=min(unroll, count))


def convert(plane, x, k, X, D, T, nj):
    tiles = T.shape[0]

    def split(i):
        rows = pl.ds(pl.multiple_of(i * 16, 16), 16)
        for t in range(tiles):
            T[t, rows, :] = plane[x, rows, pl.ds(t * LANES, LANES)]

    loop(nj // 2, split, 4)

    def body(j):
        rows = pl.ds(j, 8, stride=nj)
        row = jnp.concatenate([T[t, rows, :] for t in range(tiles)], axis=1)
        X[k, j + 1] = row
        D[k, j + 1] = rolled(row, -1, 1) - rolled(row, 1, 1)

    loop(nj, body, 16)
    fill_ends(X, k, nj)


def prepare_kernel(own, X, D, curved, rest, T):
    nj = X.shape[1] - 2
    for x in range(2):
        convert(own, x, x, X, D, T, nj)
        fill_ends(D, x, nj)

        def body(i, x=x):
            j = 2 * i
            center, beside = X[x, pl.ds(j, 4)], D[x, pl.ds(j, 4)]
            middle = center[1:3]
            double = 2.0 * middle
            curve_yy = center[2:] + center[:2] - double
            curve_zz = rolled_z(middle, 1) + rolled_z(middle, -1) - double
            cross_yz = beside[2:] - beside[:2]
            curved[x, pl.ds(j, 2)] = curve_yy + curve_zz
            rest[x, pl.ds(j, 2)] = 0.0625 * (cross_yz * cross_yz) - curve_yy * curve_zz

        loop(nj // 2, body, 8)


def source_kernel(
    X, D, curved, rest, left, right, table, f00, f01, f10, f11, s0, s1, total, XH, DH, G, T, acc
):
    nj = X.shape[1] - 2
    half = nj // 2
    outs = ((f00, f01), (f10, f11))
    convert(left, 0, 0, XH, DH, T, nj)
    convert(right, 0, 1, XH, DH, T, nj)
    lowers = ((XH, DH, 0), (X, D, 0))
    uppers = ((X, D, 1), (XH, DH, 1))
    acc[...] = jnp.zeros_like(acc)
    for x in range(2):
        for h in range(2):
            def cells(i, x=x, h=h):
                j = h * half + 2 * i
                (lower, lower_d, l), (upper, upper_d, u) = lowers[x], uppers[x]
                above, below = upper[u, pl.ds(j, 4)], lower[l, pl.ds(j, 4)]
                tilt = above - below
                curve_xx = above[1:3] + below[1:3] - 2.0 * X[x, pl.ds(j + 1, 2)]
                cross_xy = tilt[2:] - tilt[:2]
                cross_xz = upper_d[u, pl.ds(j + 1, 2)] - lower_d[l, pl.ds(j + 1, 2)]
                forcing = rest[x, pl.ds(j, 2)] + 0.0625 * (cross_xy * cross_xy + cross_xz * cross_xz)
                forcing = forcing - curve_xx * curved[x, pl.ds(j, 2)]
                outs[x][h][pl.ds(2 * i, 2)] = forcing
                pair = forcing[0] + forcing[1]
                G[x, h * (half // 2) + i] = pair
                acc[...] += pair

            loop(half // 2, cells, 4)
    folded = acc[...]
    width = folded.shape[1]
    total[...] = sum(folded[:, k : k + LANES] for k in range(0, width, LANES))
    pair_up(G, 0, table, s0)
    pair_up(G, 1, table, s1)


def load_rows(refs, V, nj):
    half = nj // 2
    for h in range(2):
        def body(i, h=h):
            V[0, h * half + i + 1] = refs[0][h][i] + refs[1][h][i]

        loop(half, body, 8)
    fill_ends(V, 0, nj)


def rhs_first_kernel(f00, f01, f10, f11, table, out, V, G):
    nj = V.shape[1] - 2
    load_rows(((f00, f01), (f10, f11)), V, nj)

    def body(i):
        center, beside = across(V, 0, 2 * i, 2)
        value = (1.0 - 5.0 * KAPPA) * center + KAPPA * beside
        G[0, i] = value[0] + value[1]

    loop(nj // 2, body, 8)
    pair_up(G, 0, table, out, 0.125)


def rhs_later_kernel(f00, f01, f10, f11, v00, v01, v10, v11, table, out, V, G):
    nj = V.shape[1] - 2
    half = nj // 2
    load_rows(((v00, v01), (v10, v11)), V, nj)
    for h in range(2):
        def body(i, h=h):
            center, beside = across(V, 0, h * half + 2 * i, 2)
            forcing = (f00, f01)[h][pl.ds(2 * i, 2)] + (f10, f11)[h][pl.ds(2 * i, 2)]
            value = forcing - (5.0 * center - beside)
            G[0, h * (half // 2) + i] = value[0] + value[1]

        loop(half // 2, body, 8)
    pair_up(G, 0, table, out, 0.125)


def correct(corrections, table, C):
    nc, nz = C.shape[1] - 2, C.shape[3]
    for k in range(3):
        block = corrections[k][...].reshape(nc * 8, nz // 2)
        C[k, pl.ds(1, nc)] = dot_exact(block, table[...], 1).reshape(nc, 8, nz)
        fill_ends(C, k, nc)


def sweep_kernel(first, *refs):
    nj = refs[-1].shape[1] - 2
    half = nj // 2
    W, part = refs[-1], refs[-2]
    start = halves(refs[:12])
    force = None if first else halves(refs[12:20])
    own, beside_weight = (1.0 - 6.0 * KAPPA, KAPPA)
    if first:
        own, beside_weight = own * KAPPA + KAPPA, KAPPA * KAPPA
    for k in range(6):
        for h in range(2):
            def fill(i, k=k, h=h):
                W[k, h * half + i + 1] = start[k][h][i]

            loop(half, fill, 8)
        if 1 <= k <= 4:
            fill_ends(W, k, nj)
    for k in range(4):
        for h in range(2):
            def body(i, k=k, h=h):
                j = h * half + 2 * i
                center, beside = across(W, k + 1, j, 2)
                at = pl.ds(j + 1, 2)
                value = own * center + beside_weight * (beside + W[k, at] + W[k + 2, at])
                if not first:
                    value = value + KAPPA * force[k][h][pl.ds(2 * i, 2)]
                part[k, pl.ds(j, 2)] = value

            loop(half // 2, body, 8)


def add_correction(part, C, V, nj):
    def body(i):
        planes = [C[a, pl.ds(i, 3)] for a in range(3)]
        centers = [plane[1] for plane in planes]
        sides = [KAPPA * (centers[a] + centers[a + 1]) for a in range(2)]
        bases = [
            (1.0 - 5.0 * KAPPA) * center + KAPPA * (rolled(center, 1, 1) + rolled(center, -1, 1)) for center in centers
        ]
        for k in range(4):
            a = (k + 1) // 2
            base = bases[a] + sides[k // 2]
            for row in range(2):
                V[k, 2 * i + row + 1] = part[k, 2 * i + row] + (base + KAPPA * planes[a][2 * row])

    loop(nj // 2, body, 4)
    for k in range(4):
        fill_ends(V, k, nj)


def residual_rows(V, force, x, h, i, half):
    j = h * half + 2 * i
    center, beside = across(V, x + 1, j, 2)
    at = pl.ds(j + 1, 2)
    beside = beside + V[x, at] + V[x + 2, at]
    return center, force[x][h][pl.ds(2 * i, 2)] - (6.0 * center - beside)


def fold_row(value):
    return jnp.sum(jnp.sum(value, axis=0, keepdims=True), axis=1, keepdims=True)


def stats_row(rest, *figures):
    lane = lax.broadcasted_iota(jnp.int32, (1, LANES), 1)
    for at, figure in enumerate(figures):
        rest = jnp.where(lane == at, figure, rest)
    return rest


def halves(refs):
    return tuple((refs[2 * k], refs[2 * k + 1]) for k in range(len(refs) // 2))


def add_figures(acc, residue, shift):
    offset = residue - shift[...][None]
    acc[0] += offset[0] + offset[1]
    acc[1] += offset[0] * offset[0] + offset[1] * offset[1]


def middle_kernel(
    f00, f01, f10, f11, part, c_own, c_left, c_right, shift, table, v00, v01, v10, v11, s0, s1, stats, V, C, G, acc
):
    nj = V.shape[1] - 2
    half = nj // 2
    force = ((f00, f01), (f10, f11))
    outs = ((v00, v01), (v10, v11))
    correct((c_left, c_own, c_right), table, C)
    add_correction(part, C, V, nj)
    acc[...] = jnp.zeros_like(acc)
    for x in range(2):
        for h in range(2):
            def body(i, x=x, h=h):
                center, residue = residual_rows(V, force, x, h, i, half)
                value = center + KAPPA * residue
                outs[x][h][pl.ds(2 * i, 2)] = value
                G[x, h * (half // 2) + i] = value[0] + value[1]
                add_figures(acc, residue, shift)

            loop(half // 2, body, 4)
    zero = jnp.zeros((1, LANES), jnp.float32)
    stats[...] = stats_row(zero, zero, zero, zero, fold_row(acc[0]), fold_row(acc[1]))
    pair_up(G, 0, table, s0)
    pair_up(G, 1, table, s1)


def last_kernel(
    f00, f01, f10, f11, part, c_own, c_left, c_right, shift, total, first, table, out, stats, V, C, acc
):
    nj = V.shape[1] - 2
    half = nj // 2
    force = ((f00, f01), (f10, f11))
    correct((c_left, c_own, c_right), table, C)
    add_correction(part, C, V, nj)
    acc[...] = jnp.zeros_like(acc)
    for x in range(2):
        for h in range(2):
            def body(i, x=x, h=h):
                center, residue = residual_rows(V, force, x, h, i, half)
                out[x, pl.ds(h * half + 2 * i, 2)] = center
                add_figures(acc, residue, shift)

            loop(half // 2, body, 4)
    row = stats_row(first[...], fold_row(total[...]), fold_row(acc[0]), fold_row(acc[1]))
    stats[...] = jnp.broadcast_to(row[None], stats.shape)


def natural_kernel(field, out, T):
    nj = field.shape[1]
    tiles = T.shape[0]
    for x in range(2):
        def body(j, x=x):
            row = field[x, j]
            for t in range(tiles):
                T[t, pl.ds(j, 8, stride=nj), :] = row[:, t * LANES : (t + 1) * LANES]

        loop(nj, body, 8)

        def join(i, x=x):
            rows = pl.ds(pl.multiple_of(i * 16, 16), 16)
            for t in range(tiles):
                out[x, rows, pl.ds(t * LANES, LANES)] = T[t, rows, :]

        loop(nj // 2, join, 4)


def finish_kernel(share, figures, field, out, norms):
    devices = figures.shape[0]
    sums = figures[:, 0:1]
    mean = -jnp.sum(sums, axis=0, keepdims=True) / (share * devices)
    off = mean + sums / share
    for c, at in enumerate((3, 1)):
        linear, square = figures[:, at : at + 1], figures[:, at + 1 : at + 2]
        squares = square + 2.0 * off * linear + share * off * off
        total = jnp.sum(squares, axis=0, keepdims=True) / (share * devices)
        norms[c] = jnp.sqrt(total)[0, 0]
    gain = mean * (CONSTANT_GAIN * CYCLES)
    for x in range(2):
        def body(i, x=x):
            rows = pl.ds(pl.multiple_of(i * 16, 16), 16)
            out[x, rows, :] = field[x, rows, :] + gain

        loop(field.shape[1] // 16, body, 4)


VMEM = pl.BlockSpec(memory_space=pltpu.VMEM)
SMEM = pl.BlockSpec(memory_space=pltpu.SMEM)


def call(kernel, args, outs, scratch, flops, out_specs=None):
    moved = 4 * (sum(a.size for a in args) + sum(int(np.prod(o)) for o in outs))
    return pl.pallas_call(
        kernel,
        out_shape=[jax.ShapeDtypeStruct(o, jnp.float32) for o in outs],
        in_specs=[VMEM] * len(args),
        out_specs=out_specs or [VMEM] * len(outs),
        scratch_shapes=[pltpu.VMEM(s, jnp.float32) for s in scratch],
        compiler_params=pltpu.CompilerParams(vmem_limit_bytes=24 * 2**20),
        cost_estimate=pl.CostEstimate(flops=flops, bytes_accessed=moved, transcendentals=0),
    )(*args)


def from_left(x):
    count = lax.axis_size("gx")
    return lax.ppermute(x, "gx", [(i, (i + 1) % count) for i in range(count)])


def from_right(x):
    count = lax.axis_size("gx")
    return lax.ppermute(x, "gx", [((i + 1) % count, i) for i in range(count)])


def gathered(rows):
    return lax.all_to_all(rows, "gx", 0, 0, tiled=True)


def coarse_beside(field):
    first, last = field[:1], field[-1:]
    below = jnp.concatenate([jnp.roll(last, 1, 1), field[:-1]], 0)
    above = jnp.concatenate([field[1:], jnp.roll(first, -1, 1)], 0)
    return below + above + jnp.roll(field, 1, 2) + jnp.roll(field, -1, 2)


def both(to_right, to_left):
    left = from_left(to_right)
    right = from_right(to_left)
    return left, right


def coarse_part(local, s0, s1, weight, chunks):
    moved = []
    left, right = both(s1, s0)
    moved.append(both(chunks[0], chunks[0]))
    rhs = local + (weight * 0.125) * (left + right)
    step = RELAX * COARSE_SCALE / 6.0
    field = step * rhs
    for sweep in range(1, COARSE):
        left, right = both(field, field)
        moved.append(both(chunks[sweep], chunks[sweep]))
        part = (1.0 - RELAX) * field + step * rhs + KAPPA * coarse_beside(field)
        field = part + KAPPA * (left + right)
    left, right = both(field, field)
    lefts, rights = zip(*moved)
    return (field, left, right), lefts, rights


def whole(potential):
    _, ny, nz = potential.shape
    nj, nc = ny // 8, ny // 16
    width = nz // 2
    share = float(potential.size)
    columns = np.arange(nz)[:, None] // 2 == np.arange(width)[None, :]
    pairs = jnp.asarray(columns, jnp.bfloat16)
    chunk = (nj // 2, 8, nz)
    coarse = (nc, 8, width)
    tall = (nj + 2, 8, nz)

    tail, potential = lax.optimization_barrier((potential[1:], potential))
    left = from_left(tail)
    right = from_right(potential[:1])
    tiles = (nz // LANES, ny, LANES)
    prepared = call(
        prepare_kernel, (potential,), [(2, *tall), (2, *tall), (2, nj, 8, nz), (2, nj, 8, nz)], [tiles], 10**8
    )
    *forcing, s0, s1, total = call(
        source_kernel, (*prepared, left, right, pairs), [chunk] * 4 + [coarse] * 2 + [(8, LANES)],
        [(2, *tall), (2, *tall), (2, nc, 8, nz), tiles, (8, nz)], 10**8,
    )
    shift = jnp.broadcast_to(jnp.sum(total) / share, (8, nz))
    (local,) = call(
        rhs_first_kernel, (*forcing, pairs), [coarse], [(1, *tall), (1, nc, 8, nz)], 3 * 10**7
    )
    correction, f_left, f_right = coarse_part(local, s0, s1, KAPPA, forcing)
    planes = (4, nj, 8, nz)
    scratch = [(4, *tall), (3, nc + 2, 8, nz)]
    (part,) = call(
        functools.partial(sweep_kernel, True), (*f_left, *forcing, *f_right), [planes], [(6, *tall)], 10**8
    )
    *field, s0, s1, first = call(
        middle_kernel, (*forcing, part, *correction, shift, pairs),
        [chunk] * 4 + [coarse] * 2 + [(1, LANES)], [*scratch, (2, nc, 8, nz), (2, 8, nz)], 10**8,
    )
    (local,) = call(
        rhs_later_kernel, (*forcing, *field, pairs), [coarse], [(1, *tall), (1, nc, 8, nz)], 3 * 10**7
    )
    correction, v_left, v_right = coarse_part(local, s0, s1, 1.0, field)
    (part,) = call(
        functools.partial(sweep_kernel, False),
        (*v_left, *field, *v_right, *f_left[2:], *forcing, *f_right[:2]), [planes], [(6, *tall)], 10**8,
    )
    result, last = call(
        last_kernel, (*forcing, part, *correction, shift, total, first, pairs),
        [(2, nj, 8, nz), (lax.axis_size("gx"), 1, LANES)], [*scratch, (2, 8, nz)], 10**8,
    )
    (result,) = call(natural_kernel, (result,), [potential.shape], [tiles], 3 * 10**7)
    result, norms = call(
        functools.partial(finish_kernel, share), (gathered(last).reshape(-1, LANES), result),
        [potential.shape, (CYCLES,)], [], 10**7, [VMEM, SMEM],
    )
    return (result, norms)


def solution(mesh):
    in_specs = (P(("runs", "gx"), None, None),)
    out_specs = (P(("runs", "gx"), None, None), P("runs"))
    return jax.shard_map(whole, mesh=mesh, in_specs=in_specs, out_specs=out_specs, check_vma=False)
```

```python
import functools

import jax
import jax.numpy as jnp
import numpy as np
from jax import lax
from jax.experimental import pallas as pl
from jax.experimental.pallas import tpu as pltpu
from jax.sharding import PartitionSpec as P

CYCLES = 2
COARSE = 4
RELAX = 0.8
KAPPA = RELAX / 6.0
COARSE_SCALE = 4.0
CONSTANT_GAIN = KAPPA * (2.0 + COARSE * COARSE_SCALE)
LANES = 128


def rolled(x, shift, axis):
    size = x.shape[axis]
    return pltpu.roll(x, shift % size, axis)


def rolled_z(x, shift):
    rows, subs, nz = x.shape
    return rolled(x.reshape(rows * subs, nz), shift, 1).reshape(x.shape)


def fill_ends(ref, plane, nj):
    ref[plane, 0] = rolled(ref[plane, nj], 1, 0)
    ref[plane, nj + 1] = rolled(ref[plane, 1], -1, 0)


def across(ref, plane, start, rows):
    wide = ref[plane, pl.ds(start, rows + 2)]
    center = wide[1 : rows + 1]
    beside = wide[:rows] + wide[2:] + rolled_z(center, 1) + rolled_z(center, -1)
    return center, beside


def dot_exact(x, table, side=0):
    high = x.astype(jnp.bfloat16)
    rest = x - high.astype(jnp.float32)
    middle = rest.astype(jnp.bfloat16)
    low = (rest - middle.astype(jnp.float32)).astype(jnp.bfloat16)
    parts = jnp.concatenate([high, middle, low], 0)
    out = lax.dot_general(parts, table, (((1,), (side,)), ((), ())), preferred_element_type=jnp.float32)
    rows = x.shape[0]
    return out[:rows] + out[rows : 2 * rows] + out[2 * rows :]


def pair_up(sums_ref, plane, table_ref, out_ref, scale=1.0):
    nc, _, nz = sums_ref.shape[1:]
    step = min(nc, 32)

    def body(i):
        at = i * step
        block = sums_ref[plane, pl.ds(at, step)].reshape(step * 8, nz)
        out = dot_exact(block, table_ref[...]) * scale
        out_ref[pl.ds(at, step)] = out.reshape(step, 8, nz // 2)

    lax.fori_loop(0, nc // step, lambda i, c: (body(i), c)[1], 0)


def loop(count, body, unroll=2):
    lax.fori_loop(0, count, lambda i, c: (body(i), c)[1], 0, unroll=min(unroll, count))


def convert(plane, x, k, X, D, T, nj):
    tiles = T.shape[0]

    def split(i):
        rows = pl.ds(pl.multiple_of(i * 16, 16), 16)
        for t in range(tiles):
            T[t, rows, :] = plane[x, rows, pl.ds(t * LANES, LANES)]

    loop(nj // 2, split, 4)

    def body(j):
        rows = pl.ds(j, 8, stride=nj)
        row = jnp.concatenate([T[t, rows, :] for t in range(tiles)], axis=1)
        X[k, j + 1] = row
        D[k, j + 1] = rolled(row, -1, 1) - rolled(row, 1, 1)

    loop(nj, body, 16)
    fill_ends(X, k, nj)


def prepare_kernel(own, X, D, curved, rest, T):
    nj = X.shape[1] - 2
    for x in range(2):
        convert(own, x, x, X, D, T, nj)
        fill_ends(D, x, nj)

        def body(i, x=x):
            j = 2 * i
            center, beside = X[x, pl.ds(j, 4)], D[x, pl.ds(j, 4)]
            middle = center[1:3]
            double = 2.0 * middle
            curve_yy = center[2:] + center[:2] - double
            curve_zz = rolled_z(middle, 1) + rolled_z(middle, -1) - double
            cross_yz = beside[2:] - beside[:2]
            curved[x, pl.ds(j, 2)] = curve_yy + curve_zz
            rest[x, pl.ds(j, 2)] = 0.0625 * (cross_yz * cross_yz) - curve_yy * curve_zz

        loop(nj // 2, body, 8)


def source_kernel(
    X, D, curved, rest, left, right, table, f00, f01, f10, f11, s0, s1, total, XH, DH, G, T, acc
):
    nj = X.shape[1] - 2
    half = nj // 2
    outs = ((f00, f01), (f10, f11))
    convert(left, 0, 0, XH, DH, T, nj)
    convert(right, 0, 1, XH, DH, T, nj)
    lowers = ((XH, DH, 0), (X, D, 0))
    uppers = ((X, D, 1), (XH, DH, 1))
    acc[...] = jnp.zeros_like(acc)
    for x in range(2):
        for h in range(2):
            def cells(i, x=x, h=h):
                j = h * half + 2 * i
                (lower, lower_d, l), (upper, upper_d, u) = lowers[x], uppers[x]
                above, below = upper[u, pl.ds(j, 4)], lower[l, pl.ds(j, 4)]
                tilt = above - below
                curve_xx = above[1:3] + below[1:3] - 2.0 * X[x, pl.ds(j + 1, 2)]
                cross_xy = tilt[2:] - tilt[:2]
                cross_xz = upper_d[u, pl.ds(j + 1, 2)] - lower_d[l, pl.ds(j + 1, 2)]
                forcing = rest[x, pl.ds(j, 2)] + 0.0625 * (cross_xy * cross_xy + cross_xz * cross_xz)
                forcing = forcing - curve_xx * curved[x, pl.ds(j, 2)]
                outs[x][h][pl.ds(2 * i, 2)] = forcing
                pair = forcing[0] + forcing[1]
                G[x, h * (half // 2) + i] = pair
                acc[...] += pair

            loop(half // 2, cells, 4)
    folded = acc[...]
    width = folded.shape[1]
    total[...] = sum(folded[:, k : k + LANES] for k in range(0, width, LANES))
    pair_up(G, 0, table, s0)
    pair_up(G, 1, table, s1)


def load_rows(refs, V, nj):
    half = nj // 2
    for h in range(2):
        def body(i, h=h):
            V[0, h * half + i + 1] = refs[0][h][i] + refs[1][h][i]

        loop(half, body, 8)
    fill_ends(V, 0, nj)


def rhs_first_kernel(f00, f01, f10, f11, table, out, V, G):
    nj = V.shape[1] - 2
    load_rows(((f00, f01), (f10, f11)), V, nj)

    def body(i):
        center, beside = across(V, 0, 2 * i, 2)
        value = (1.0 - 5.0 * KAPPA) * center + KAPPA * beside
        G[0, i] = value[0] + value[1]

    loop(nj // 2, body, 8)
    pair_up(G, 0, table, out, 0.125)


def rhs_later_kernel(f00, f01, f10, f11, v00, v01, v10, v11, table, out, V, G):
    nj = V.shape[1] - 2
    half = nj // 2
    load_rows(((v00, v01), (v10, v11)), V, nj)
    for h in range(2):
        def body(i, h=h):
            center, beside = across(V, 0, h * half + 2 * i, 2)
            forcing = (f00, f01)[h][pl.ds(2 * i, 2)] + (f10, f11)[h][pl.ds(2 * i, 2)]
            value = forcing - (5.0 * center - beside)
            G[0, h * (half // 2) + i] = value[0] + value[1]

        loop(half // 2, body, 8)
    pair_up(G, 0, table, out, 0.125)


def correct(corrections, table, C):
    nc, nz = C.shape[1] - 2, C.shape[3]
    for k in range(3):
        block = corrections[k][...].reshape(nc * 8, nz // 2)
        C[k, pl.ds(1, nc)] = dot_exact(block, table[...], 1).reshape(nc, 8, nz)
        fill_ends(C, k, nc)


def sweep_weights(first):
    own, beside = 1.0 - 6.0 * KAPPA, KAPPA
    return ((own + 1.0) * KAPPA, KAPPA * KAPPA) if first else (own, beside)


def fill_planes(start, W, nj):
    half = nj // 2
    for k, plane in enumerate(start):
        for h in range(2):
            def fill(i, k=k, h=h, plane=plane):
                W[k, h * half + i + 1] = plane[h][i]

            loop(half, fill, 8)
        fill_ends(W, k, nj)


def own_sweep_kernel(first, *refs):
    out, W = refs[-2:]
    nj = W.shape[1] - 2
    half = nj // 2
    start = halves(refs[:4])
    force = None if first else halves(refs[4:8])
    own, weight = sweep_weights(first)
    fill_planes(start, W, nj)
    for x in range(2):
        for h in range(2):
            def body(i, x=x, h=h):
                j = h * half + 2 * i
                center, beside = across(W, x, j, 2)
                value = own * center + weight * (beside + W[1 - x, pl.ds(j + 1, 2)])
                if not first:
                    value = value + KAPPA * force[x][h][pl.ds(2 * i, 2)]
                out[x, pl.ds(j, 2)] = value

            loop(half // 2, body, 8)


def sweep_kernel(first, *refs):
    inner, part, W = refs[-3:]
    nj = W.shape[1] - 2
    half = nj // 2
    start = halves(refs[:12])
    force = None if first else halves(refs[12:16])
    own, weight = sweep_weights(first)
    fill_planes((start[1], start[4]), W, nj)
    for side, (k, below, above) in enumerate(((0, 0, 2), (3, 3, 5))):
        for h in range(2):
            def outer(i, side=side, k=k, below=below, above=above, h=h):
                j = h * half + 2 * i
                at = pl.ds(2 * i, 2)
                center, beside = across(W, side, j, 2)
                value = own * center + weight * (beside + start[below][h][at] + start[above][h][at])
                if not first:
                    value = value + KAPPA * force[side][h][at]
                part[k, pl.ds(j, 2)] = value

            loop(half // 2, outer, 8)
    for x, k in enumerate((1, 4)):
        for h in range(2):
            def border(i, x=x, k=k, h=h):
                j = h * half + 2 * i
                part[x + 1, pl.ds(j, 2)] = inner[x, pl.ds(j, 2)] + weight * start[k][h][pl.ds(2 * i, 2)]

            loop(half // 2, border, 8)


def add_correction(part, C, V, nj):
    def body(i):
        planes = [C[a, pl.ds(i, 3)] for a in range(3)]
        centers = [plane[1] for plane in planes]
        sides = [KAPPA * (centers[a] + centers[a + 1]) for a in range(2)]
        bases = [
            (1.0 - 5.0 * KAPPA) * center + KAPPA * (rolled(center, 1, 1) + rolled(center, -1, 1)) for center in centers
        ]
        for k in range(4):
            a = (k + 1) // 2
            base = bases[a] + sides[k // 2]
            for row in range(2):
                V[k, 2 * i + row + 1] = part[k, 2 * i + row] + (base + KAPPA * planes[a][2 * row])

    loop(nj // 2, body, 4)
    for k in range(4):
        fill_ends(V, k, nj)


def residual_rows(V, force, x, h, i, half):
    j = h * half + 2 * i
    center, beside = across(V, x + 1, j, 2)
    at = pl.ds(j + 1, 2)
    beside = beside + V[x, at] + V[x + 2, at]
    return center, force[x][h][pl.ds(2 * i, 2)] - (6.0 * center - beside)


def fold_row(value):
    return jnp.sum(jnp.sum(value, axis=0, keepdims=True), axis=1, keepdims=True)


def stats_row(rest, *figures):
    lane = lax.broadcasted_iota(jnp.int32, (1, LANES), 1)
    for at, figure in enumerate(figures):
        rest = jnp.where(lane == at, figure, rest)
    return rest


def halves(refs):
    return tuple((refs[2 * k], refs[2 * k + 1]) for k in range(len(refs) // 2))


def add_figures(acc, residue, shift):
    offset = residue - shift[...][None]
    acc[0] += offset[0] + offset[1]
    acc[1] += offset[0] * offset[0] + offset[1] * offset[1]


def middle_kernel(
    f00, f01, f10, f11, part, c_own, c_left, c_right, shift, table, v00, v01, v10, v11, s0, s1, stats, V, C, G, acc
):
    nj = V.shape[1] - 2
    half = nj // 2
    force = ((f00, f01), (f10, f11))
    outs = ((v00, v01), (v10, v11))
    correct((c_left, c_own, c_right), table, C)
    add_correction(part, C, V, nj)
    acc[...] = jnp.zeros_like(acc)
    for x in range(2):
        for h in range(2):
            def body(i, x=x, h=h):
                center, residue = residual_rows(V, force, x, h, i, half)
                value = center + KAPPA * residue
                outs[x][h][pl.ds(2 * i, 2)] = value
                G[x, h * (half // 2) + i] = value[0] + value[1]
                add_figures(acc, residue, shift)

            loop(half // 2, body, 4)
    zero = jnp.zeros((1, LANES), jnp.float32)
    stats[...] = stats_row(zero, zero, zero, zero, fold_row(acc[0]), fold_row(acc[1]))
    pair_up(G, 0, table, s0)
    pair_up(G, 1, table, s1)


def last_kernel(
    f00, f01, f10, f11, part, c_own, c_left, c_right, shift, total, first, table, out, stats, V, C, acc
):
    nj = V.shape[1] - 2
    half = nj // 2
    force = ((f00, f01), (f10, f11))
    correct((c_left, c_own, c_right), table, C)
    add_correction(part, C, V, nj)
    acc[...] = jnp.zeros_like(acc)
    for x in range(2):
        for h in range(2):
            def body(i, x=x, h=h):
                center, residue = residual_rows(V, force, x, h, i, half)
                for row in range(2):
                    for t in range(out.shape[1]):
                        cells = center[row, :, t * LANES : (t + 1) * LANES]
                        out[x, t, pl.ds(h * half + 2 * i + row, 8, stride=nj), :] = cells
                add_figures(acc, residue, shift)

            loop(half // 2, body, 4)
    row = stats_row(first[...], fold_row(total[...]), fold_row(acc[0]), fold_row(acc[1]))
    stats[...] = jnp.broadcast_to(row[None], stats.shape)


def finish_kernel(share, figures, field, out, norms, gain_ref):
    devices = figures.shape[0]

    @pl.when(pl.program_id(0) == 0)
    def _():
        sums = figures[:, 0:1]
        mean = -jnp.sum(sums, axis=0, keepdims=True) / (share * devices)
        off = mean + sums / share
        for c, at in enumerate((3, 1)):
            linear, square = figures[:, at : at + 1], figures[:, at + 1 : at + 2]
            squares = square + 2.0 * off * linear + share * off * off
            total = jnp.sum(squares, axis=0, keepdims=True) / (share * devices)
            norms[c] = jnp.sqrt(total)[0, 0]
        gain_ref[...] = jnp.broadcast_to(mean * (CONSTANT_GAIN * CYCLES), gain_ref.shape)

    gain = gain_ref[...]
    for x in range(2):
        def body(i, x=x):
            rows = pl.ds(pl.multiple_of(i * 16, 16), 16)
            for t in range(field.shape[1]):
                out[x, rows, pl.ds(t * LANES, LANES)] = field[x, t, rows, :] + gain[:1]

        loop(field.shape[2] // 16, body, 4)


VMEM = pl.BlockSpec(memory_space=pltpu.VMEM)
SMEM = pl.BlockSpec(memory_space=pltpu.SMEM)


def call(kernel, args, outs, scratch, flops, out_specs=None):
    moved = 4 * (sum(a.size for a in args) + sum(int(np.prod(o)) for o in outs))
    return pl.pallas_call(
        kernel,
        out_shape=[jax.ShapeDtypeStruct(o, jnp.float32) for o in outs],
        in_specs=[VMEM] * len(args),
        out_specs=out_specs or [VMEM] * len(outs),
        scratch_shapes=[pltpu.VMEM(s, jnp.float32) for s in scratch],
        compiler_params=pltpu.CompilerParams(vmem_limit_bytes=24 * 2**20),
        cost_estimate=pl.CostEstimate(flops=flops, bytes_accessed=moved, transcendentals=0),
    )(*args)


def from_left(x):
    count = lax.axis_size("gx")
    return lax.ppermute(x, "gx", [(i, (i + 1) % count) for i in range(count)])


def from_right(x):
    count = lax.axis_size("gx")
    return lax.ppermute(x, "gx", [((i + 1) % count, i) for i in range(count)])


def gathered(rows):
    return lax.all_to_all(rows, "gx", 0, 0, tiled=True)


def coarse_beside(field):
    first, last = field[:1], field[-1:]
    below = jnp.concatenate([jnp.roll(last, 1, 1), field[:-1]], 0)
    above = jnp.concatenate([field[1:], jnp.roll(first, -1, 1)], 0)
    return below + above + jnp.roll(field, 1, 2) + jnp.roll(field, -1, 2)


def both(to_right, to_left):
    left = from_left(to_right)
    right = from_right(to_left)
    return left, right


def coarse_part(local, s0, s1, weight, chunks, force, shape):
    moved = []
    left, right = both(s1, s0)
    moved.append(both(chunks[0], chunks[0]))
    rhs = local + (weight * 0.125) * (left + right)
    step = RELAX * COARSE_SCALE / 6.0
    field = step * rhs
    for sweep in range(1, COARSE):
        left, right = both(field, field)
        moved.append(both(chunks[sweep], chunks[sweep]))
        part = (1.0 - RELAX) * field + step * rhs + KAPPA * coarse_beside(field)
        field = part + KAPPA * (left + right)
    left, right = both(field, field)
    lefts, rights = zip(*moved)
    (inner,) = call(
        functools.partial(own_sweep_kernel, not force), (*chunks, *force), [(2, *shape)],
        [(2, shape[0] + 2, *shape[1:])], 10**8,
    )
    return (field, left, right), lefts, rights, inner


def whole(potential):
    _, ny, nz = potential.shape
    nj, nc = ny // 8, ny // 16
    width = nz // 2
    share = float(potential.size)
    columns = np.arange(nz)[:, None] // 2 == np.arange(width)[None, :]
    pairs = jnp.asarray(columns, jnp.bfloat16)
    chunk = (nj // 2, 8, nz)
    coarse = (nc, 8, width)
    tall = (nj + 2, 8, nz)

    tail, potential = lax.optimization_barrier((potential[1:], potential))
    left = from_left(tail)
    right = from_right(potential[:1])
    tiles = (nz // LANES, ny, LANES)
    prepared = call(
        prepare_kernel, (potential,), [(2, *tall), (2, *tall), (2, nj, 8, nz), (2, nj, 8, nz)], [tiles], 10**8
    )
    *forcing, s0, s1, total = call(
        source_kernel, (*prepared, left, right, pairs), [chunk] * 4 + [coarse] * 2 + [(8, LANES)],
        [(2, *tall), (2, *tall), (2, nc, 8, nz), tiles, (8, nz)], 10**8,
    )
    shift = jnp.broadcast_to(jnp.sum(total) / share, (8, nz))
    (local,) = call(
        rhs_first_kernel, (*forcing, pairs), [coarse], [(1, *tall), (1, nc, 8, nz)], 3 * 10**7
    )
    rows = (nj, 8, nz)
    correction, f_left, f_right, inner = coarse_part(local, s0, s1, KAPPA, forcing, (), rows)
    planes = (4, nj, 8, nz)
    scratch = [(4, *tall), (3, nc + 2, 8, nz)]
    (part,) = call(
        functools.partial(sweep_kernel, True), (*f_left, *forcing, *f_right, inner), [planes], [(2, *tall)], 10**8
    )
    *field, s0, s1, first = call(
        middle_kernel, (*forcing, part, *correction, shift, pairs),
        [chunk] * 4 + [coarse] * 2 + [(1, LANES)], [*scratch, (2, nc, 8, nz), (2, 8, nz)], 10**8,
    )
    (local,) = call(
        rhs_later_kernel, (*forcing, *field, pairs), [coarse], [(1, *tall), (1, nc, 8, nz)], 3 * 10**7
    )
    correction, v_left, v_right, inner = coarse_part(local, s0, s1, 1.0, field, forcing, rows)
    (part,) = call(
        functools.partial(sweep_kernel, False),
        (*v_left, *field, *v_right, *f_left[2:], *f_right[:2], inner), [planes], [(2, *tall)], 10**8,
    )
    result, last = call(
        last_kernel, (*forcing, part, *correction, shift, total, first, pairs),
        [(2, *tiles), (lax.axis_size("gx"), 1, LANES)], [*scratch, (2, 8, nz)], 10**8,
    )
    figures = gathered(last).reshape(-1, LANES)
    blocks = 2
    count = nz // LANES
    result, norms = pl.pallas_call(
        functools.partial(finish_kernel, share),
        grid=(blocks,),
        out_shape=[jax.ShapeDtypeStruct(potential.shape, jnp.float32), jax.ShapeDtypeStruct((CYCLES,), jnp.float32)],
        in_specs=[
            pl.BlockSpec(figures.shape, lambda i: (0, 0)),
            pl.BlockSpec((2, count, ny // blocks, LANES), lambda i: (0, 0, i, 0)),
        ],
        out_specs=[pl.BlockSpec((2, ny // blocks, nz), lambda i: (0, i, 0)), SMEM],
        scratch_shapes=[pltpu.VMEM((8, LANES), jnp.float32)],
        compiler_params=pltpu.CompilerParams(vmem_limit_bytes=16 * 2**20),
        cost_estimate=pl.CostEstimate(flops=10**7, bytes_accessed=8 * result.size, transcendentals=0),
    )(figures, result)
    return (result, norms)


def solution(mesh):
    in_specs = (P(("runs", "gx"), None, None),)
    out_specs = (P(("runs", "gx"), None, None), P("runs"))
    return jax.shard_map(whole, mesh=mesh, in_specs=in_specs, out_specs=out_specs, check_vma=False)
```

```python
import functools

import jax
import jax.numpy as jnp
import numpy as np
from jax import lax
from jax.experimental import pallas as pl
from jax.experimental.pallas import tpu as pltpu
from jax.sharding import PartitionSpec as P

CYCLES = 2
COARSE = 4
RELAX = 0.8
KAPPA = RELAX / 6.0
COARSE_SCALE = 4.0
CONSTANT_GAIN = KAPPA * (2.0 + COARSE * COARSE_SCALE)
LANES = 128


def rolled(x, shift, axis):
    size = x.shape[axis]
    return pltpu.roll(x, shift % size, axis)


def rolled_z(x, shift):
    rows, subs, nz = x.shape
    return rolled(x.reshape(rows * subs, nz), shift, 1).reshape(x.shape)


def fill_ends(ref, plane, nj):
    ref[plane, 0] = rolled(ref[plane, nj], 1, 0)
    ref[plane, nj + 1] = rolled(ref[plane, 1], -1, 0)


def across(ref, plane, start, rows):
    wide = ref[plane, pl.ds(start, rows + 2)]
    center = wide[1 : rows + 1]
    beside = wide[:rows] + wide[2:] + rolled_z(center, 1) + rolled_z(center, -1)
    return center, beside


def dot_exact(x, table, side=0):
    high = x.astype(jnp.bfloat16)
    rest = x - high.astype(jnp.float32)
    middle = rest.astype(jnp.bfloat16)
    low = (rest - middle.astype(jnp.float32)).astype(jnp.bfloat16)
    parts = jnp.concatenate([high, middle, low], 0)
    out = lax.dot_general(parts, table, (((1,), (side,)), ((), ())), preferred_element_type=jnp.float32)
    rows = x.shape[0]
    return out[:rows] + out[rows : 2 * rows] + out[2 * rows :]


def pair_up(sums_ref, plane, table_ref, out_ref, scale=1.0):
    nc, _, nz = sums_ref.shape[1:]
    step = min(nc, 32)

    def body(i):
        at = i * step
        block = sums_ref[plane, pl.ds(at, step)].reshape(step * 8, nz)
        out = dot_exact(block, table_ref[...]) * scale
        out_ref[pl.ds(at, step)] = out.reshape(step, 8, nz // 2)

    lax.fori_loop(0, nc // step, lambda i, c: (body(i), c)[1], 0)


def loop(count, body, unroll=2):
    lax.fori_loop(0, count, lambda i, c: (body(i), c)[1], 0, unroll=min(unroll, count))


def convert(plane, x, k, X, D, T, nj):
    tiles = T.shape[0]

    def split(i):
        rows = pl.ds(pl.multiple_of(i * 16, 16), 16)
        for t in range(tiles):
            T[t, rows, :] = plane[x, rows, pl.ds(t * LANES, LANES)]

    loop(nj // 2, split, 4)

    def body(j):
        rows = pl.ds(j, 8, stride=nj)
        row = jnp.concatenate([T[t, rows, :] for t in range(tiles)], axis=1)
        X[k, j + 1] = row
        D[k, j + 1] = rolled(row, -1, 1) - rolled(row, 1, 1)

    loop(nj, body, 16)
    fill_ends(X, k, nj)


def prepare_kernel(own, X, D, curved, rest, T):
    nj = X.shape[1] - 2
    for x in range(2):
        convert(own, x, x, X, D, T, nj)
        fill_ends(D, x, nj)

        def body(i, x=x):
            j = 2 * i
            center, beside = X[x, pl.ds(j, 4)], D[x, pl.ds(j, 4)]
            middle = center[1:3]
            double = 2.0 * middle
            curve_yy = center[2:] + center[:2] - double
            curve_zz = rolled_z(middle, 1) + rolled_z(middle, -1) - double
            cross_yz = beside[2:] - beside[:2]
            curved[x, pl.ds(j, 2)] = curve_yy + curve_zz
            rest[x, pl.ds(j, 2)] = 0.0625 * (cross_yz * cross_yz) - curve_yy * curve_zz

        loop(nj // 2, body, 8)


def source_kernel(
    X, D, curved, rest, left, right, table, f00, f01, f10, f11, s0, s1, total, shift, XH, DH, G, T, acc
):
    nj = X.shape[1] - 2
    half = nj // 2
    outs = ((f00, f01), (f10, f11))
    convert(left, 0, 0, XH, DH, T, nj)
    convert(right, 0, 1, XH, DH, T, nj)
    lowers = ((XH, DH, 0), (X, D, 0))
    uppers = ((X, D, 1), (XH, DH, 1))
    acc[...] = jnp.zeros_like(acc)
    for x in range(2):
        for h in range(2):
            def cells(i, x=x, h=h):
                j = h * half + 2 * i
                (lower, lower_d, l), (upper, upper_d, u) = lowers[x], uppers[x]
                above, below = upper[u, pl.ds(j, 4)], lower[l, pl.ds(j, 4)]
                tilt = above - below
                curve_xx = above[1:3] + below[1:3] - 2.0 * X[x, pl.ds(j + 1, 2)]
                cross_xy = tilt[2:] - tilt[:2]
                cross_xz = upper_d[u, pl.ds(j + 1, 2)] - lower_d[l, pl.ds(j + 1, 2)]
                forcing = rest[x, pl.ds(j, 2)] + 0.0625 * (cross_xy * cross_xy + cross_xz * cross_xz)
                forcing = forcing - curve_xx * curved[x, pl.ds(j, 2)]
                outs[x][h][pl.ds(2 * i, 2)] = forcing
                pair = forcing[0] + forcing[1]
                G[x, h * (half // 2) + i] = pair
                acc[...] += pair

            loop(half // 2, cells, 4)
    folded = acc[...]
    width = folded.shape[1]
    total[...] = sum(folded[:, k : k + LANES] for k in range(0, width, LANES))
    shift[...] = jnp.broadcast_to(fold_row(total[...]) * (1.0 / (2 * nj * acc.size)), shift.shape)
    pair_up(G, 0, table, s0)
    pair_up(G, 1, table, s1)


def load_rows(refs, V, nj):
    half = nj // 2
    for h in range(2):
        def body(i, h=h):
            V[0, h * half + i + 1] = refs[0][h][i] + refs[1][h][i]

        loop(half, body, 8)
    fill_ends(V, 0, nj)


def rhs_first_kernel(f00, f01, f10, f11, table, out, V, G):
    nj = V.shape[1] - 2
    load_rows(((f00, f01), (f10, f11)), V, nj)

    def body(i):
        center, beside = across(V, 0, 2 * i, 2)
        value = (1.0 - 5.0 * KAPPA) * center + KAPPA * beside
        G[0, i] = value[0] + value[1]

    loop(nj // 2, body, 8)
    pair_up(G, 0, table, out, 0.125)


def rhs_later_kernel(f00, f01, f10, f11, v00, v01, v10, v11, table, out, V, G):
    nj = V.shape[1] - 2
    half = nj // 2
    load_rows(((v00, v01), (v10, v11)), V, nj)
    for h in range(2):
        def body(i, h=h):
            center, beside = across(V, 0, h * half + 2 * i, 2)
            forcing = (f00, f01)[h][pl.ds(2 * i, 2)] + (f10, f11)[h][pl.ds(2 * i, 2)]
            value = forcing - (5.0 * center - beside)
            G[0, h * (half // 2) + i] = value[0] + value[1]

        loop(half // 2, body, 8)
    pair_up(G, 0, table, out, 0.125)


def correct(corrections, table, C):
    nc, nz = C.shape[1] - 2, C.shape[3]
    for k in range(3):
        block = corrections[k][...].reshape(nc * 8, nz // 2)
        C[k, pl.ds(1, nc)] = dot_exact(block, table[...], 1).reshape(nc, 8, nz)
        fill_ends(C, k, nc)


def sweep_weights(first):
    own, beside = 1.0 - 6.0 * KAPPA, KAPPA
    return ((own + 1.0) * KAPPA, KAPPA * KAPPA) if first else (own, beside)


def fill_planes(start, W, nj):
    half = nj // 2
    for k, plane in enumerate(start):
        for h in range(2):
            def fill(i, k=k, h=h, plane=plane):
                W[k, h * half + i + 1] = plane[h][i]

            loop(half, fill, 8)
        fill_ends(W, k, nj)


def own_sweep_kernel(first, *refs):
    out, W = refs[-2:]
    nj = W.shape[1] - 2
    half = nj // 2
    start = halves(refs[:4])
    force = None if first else halves(refs[4:8])
    own, weight = sweep_weights(first)
    fill_planes(start, W, nj)
    for x in range(2):
        for h in range(2):
            def body(i, x=x, h=h):
                j = h * half + 2 * i
                center, beside = across(W, x, j, 2)
                value = own * center + weight * (beside + W[1 - x, pl.ds(j + 1, 2)])
                if not first:
                    value = value + KAPPA * force[x][h][pl.ds(2 * i, 2)]
                out[x, pl.ds(j, 2)] = value

            loop(half // 2, body, 8)


def sweep_kernel(first, *refs):
    inner, part, W = refs[-3:]
    nj = W.shape[1] - 2
    half = nj // 2
    start = halves(refs[:12])
    force = None if first else halves(refs[12:16])
    own, weight = sweep_weights(first)
    fill_planes((start[1], start[4]), W, nj)
    for side, (k, below, above) in enumerate(((0, 0, 2), (3, 3, 5))):
        for h in range(2):
            def outer(i, side=side, k=k, below=below, above=above, h=h):
                j = h * half + 2 * i
                at = pl.ds(2 * i, 2)
                center, beside = across(W, side, j, 2)
                value = own * center + weight * (beside + start[below][h][at] + start[above][h][at])
                if not first:
                    value = value + KAPPA * force[side][h][at]
                part[k, pl.ds(j, 2)] = value

            loop(half // 2, outer, 8)
    for x, k in enumerate((1, 4)):
        for h in range(2):
            def border(i, x=x, k=k, h=h):
                j = h * half + 2 * i
                part[x + 1, pl.ds(j, 2)] = inner[x, pl.ds(j, 2)] + weight * start[k][h][pl.ds(2 * i, 2)]

            loop(half // 2, border, 8)


def add_correction(part, C, V, nj):
    def body(i):
        planes = [C[a, pl.ds(i, 3)] for a in range(3)]
        centers = [plane[1] for plane in planes]
        sides = [KAPPA * (centers[a] + centers[a + 1]) for a in range(2)]
        bases = [
            (1.0 - 5.0 * KAPPA) * center + KAPPA * (rolled(center, 1, 1) + rolled(center, -1, 1)) for center in centers
        ]
        for k in range(4):
            a = (k + 1) // 2
            base = bases[a] + sides[k // 2]
            for row in range(2):
                V[k, 2 * i + row + 1] = part[k, 2 * i + row] + (base + KAPPA * planes[a][2 * row])

    loop(nj // 2, body, 4)
    for k in range(4):
        fill_ends(V, k, nj)


def residual_rows(V, force, x, h, i, half):
    j = h * half + 2 * i
    center, beside = across(V, x + 1, j, 2)
    at = pl.ds(j + 1, 2)
    beside = beside + V[x, at] + V[x + 2, at]
    return center, force[x][h][pl.ds(2 * i, 2)] - (6.0 * center - beside)


def fold_row(value):
    return jnp.sum(jnp.sum(value, axis=0, keepdims=True), axis=1, keepdims=True)


def stats_row(rest, *figures):
    lane = lax.broadcasted_iota(jnp.int32, (1, LANES), 1)
    for at, figure in enumerate(figures):
        rest = jnp.where(lane == at, figure, rest)
    return rest


def halves(refs):
    return tuple((refs[2 * k], refs[2 * k + 1]) for k in range(len(refs) // 2))


def add_figures(acc, residue, shift):
    offset = residue - shift[...][None]
    acc[0] += offset[0] + offset[1]
    acc[1] += offset[0] * offset[0] + offset[1] * offset[1]


def middle_kernel(
    f00, f01, f10, f11, part, c_own, c_left, c_right, shift, table, v00, v01, v10, v11, s0, s1, stats, V, C, G, acc
):
    nj = V.shape[1] - 2
    half = nj // 2
    force = ((f00, f01), (f10, f11))
    outs = ((v00, v01), (v10, v11))
    correct((c_left, c_own, c_right), table, C)
    add_correction(part, C, V, nj)
    acc[...] = jnp.zeros_like(acc)
    for x in range(2):
        for h in range(2):
            def body(i, x=x, h=h):
                center, residue = residual_rows(V, force, x, h, i, half)
                value = center + KAPPA * residue
                outs[x][h][pl.ds(2 * i, 2)] = value
                G[x, h * (half // 2) + i] = value[0] + value[1]
                add_figures(acc, residue, shift)

            loop(half // 2, body, 4)
    zero = jnp.zeros((1, LANES), jnp.float32)
    stats[...] = stats_row(zero, zero, zero, zero, fold_row(acc[0]), fold_row(acc[1]))
    pair_up(G, 0, table, s0)
    pair_up(G, 1, table, s1)


def last_kernel(
    f00, f01, f10, f11, part, c_own, c_left, c_right, shift, total, first, table, out, stats, V, C, acc
):
    nj = V.shape[1] - 2
    half = nj // 2
    force = ((f00, f01), (f10, f11))
    correct((c_left, c_own, c_right), table, C)
    add_correction(part, C, V, nj)
    acc[...] = jnp.zeros_like(acc)
    for x in range(2):
        for h in range(2):
            def body(i, x=x, h=h):
                center, residue = residual_rows(V, force, x, h, i, half)
                for row in range(2):
                    for t in range(out.shape[1]):
                        cells = center[row, :, t * LANES : (t + 1) * LANES]
                        out[x, t, pl.ds(h * half + 2 * i + row, 8, stride=nj), :] = cells
                add_figures(acc, residue, shift)

            loop(half // 2, body, 4)
    row = stats_row(first[...], fold_row(total[...]), fold_row(acc[0]), fold_row(acc[1]))
    stats[...] = jnp.broadcast_to(row[None], stats.shape)


def finish_kernel(share, figures, field, out, norms, gain_ref):
    devices = figures.shape[0]

    @pl.when(pl.program_id(0) == 0)
    def _():
        sums = figures[:, 0:1]
        mean = -jnp.sum(sums, axis=0, keepdims=True) / (share * devices)
        off = mean + sums / share
        for c, at in enumerate((3, 1)):
            linear, square = figures[:, at : at + 1], figures[:, at + 1 : at + 2]
            squares = square + 2.0 * off * linear + share * off * off
            total = jnp.sum(squares, axis=0, keepdims=True) / (share * devices)
            norms[c] = jnp.sqrt(total)[0, 0]
        gain_ref[...] = jnp.broadcast_to(mean * (CONSTANT_GAIN * CYCLES), gain_ref.shape)

    gain = gain_ref[...]
    for x in range(2):
        def body(i, x=x):
            rows = pl.ds(pl.multiple_of(i * 16, 16), 16)
            for t in range(field.shape[1]):
                out[x, rows, pl.ds(t * LANES, LANES)] = field[x, t, rows, :] + gain[:1]

        loop(field.shape[2] // 16, body, 4)


VMEM = pl.BlockSpec(memory_space=pltpu.VMEM)
SMEM = pl.BlockSpec(memory_space=pltpu.SMEM)


def call(kernel, args, outs, scratch, flops, out_specs=None):
    moved = 4 * (sum(a.size for a in args) + sum(int(np.prod(o)) for o in outs))
    return pl.pallas_call(
        kernel,
        out_shape=[jax.ShapeDtypeStruct(o, jnp.float32) for o in outs],
        in_specs=[VMEM] * len(args),
        out_specs=out_specs or [VMEM] * len(outs),
        scratch_shapes=[pltpu.VMEM(s, jnp.float32) for s in scratch],
        compiler_params=pltpu.CompilerParams(vmem_limit_bytes=20 * 2**20),
        cost_estimate=pl.CostEstimate(flops=flops, bytes_accessed=moved, transcendentals=0),
    )(*args)


def from_left(x):
    count = lax.axis_size("gx")
    return lax.ppermute(x, "gx", [(i, (i + 1) % count) for i in range(count)])


def from_right(x):
    count = lax.axis_size("gx")
    return lax.ppermute(x, "gx", [((i + 1) % count, i) for i in range(count)])


def gathered(rows):
    return lax.all_to_all(rows, "gx", 0, 0, tiled=True)


def coarse_beside(field):
    first, last = field[:1], field[-1:]
    below = jnp.concatenate([jnp.roll(last, 1, 1), field[:-1]], 0)
    above = jnp.concatenate([field[1:], jnp.roll(first, -1, 1)], 0)
    return below + above + jnp.roll(field, 1, 2) + jnp.roll(field, -1, 2)


def both(to_right, to_left):
    left = from_left(to_right)
    right = from_right(to_left)
    return left, right


def coarse_part(local, s0, s1, weight, chunks, force, shape):
    moved = []
    left, right = both(s1, s0)
    moved.append(both(chunks[0], chunks[0]))
    rhs = local + (weight * 0.125) * (left + right)
    step = RELAX * COARSE_SCALE / 6.0
    field = step * rhs
    for sweep in range(1, COARSE):
        left, right = both(field, field)
        moved.append(both(chunks[sweep], chunks[sweep]))
        part = (1.0 - RELAX) * field + step * rhs + KAPPA * coarse_beside(field)
        field = part + KAPPA * (left + right)
    left, right = both(field, field)
    lefts, rights = zip(*moved)
    (inner,) = call(
        functools.partial(own_sweep_kernel, not force), (*chunks, *force), [(2, *shape)],
        [(2, shape[0] + 2, *shape[1:])], 10**8,
    )
    return (field, left, right), lefts, rights, inner


def whole(potential):
    _, ny, nz = potential.shape
    nj, nc = ny // 8, ny // 16
    width = nz // 2
    share = float(potential.size)
    columns = np.arange(nz)[:, None] // 2 == np.arange(width)[None, :]
    pairs = jnp.asarray(columns, jnp.bfloat16)
    chunk = (nj // 2, 8, nz)
    coarse = (nc, 8, width)
    tall = (nj + 2, 8, nz)

    tail, potential = lax.optimization_barrier((potential[1:], potential))
    left = from_left(tail)
    right = from_right(potential[:1])
    tiles = (nz // LANES, ny, LANES)
    prepared = call(
        prepare_kernel, (potential,), [(2, *tall), (2, *tall), (2, nj, 8, nz), (2, nj, 8, nz)], [tiles], 10**8
    )
    *forcing, s0, s1, total, shift = call(
        source_kernel, (*prepared, left, right, pairs), [chunk] * 4 + [coarse] * 2 + [(8, LANES), (8, nz)],
        [(2, *tall), (2, *tall), (2, nc, 8, nz), tiles, (8, nz)], 10**8,
    )
    (local,) = call(
        rhs_first_kernel, (*forcing, pairs), [coarse], [(1, *tall), (1, nc, 8, nz)], 3 * 10**7
    )
    rows = (nj, 8, nz)
    correction, f_left, f_right, inner = coarse_part(local, s0, s1, KAPPA, forcing, (), rows)
    planes = (4, nj, 8, nz)
    scratch = [(4, *tall), (3, nc + 2, 8, nz)]
    (part,) = call(
        functools.partial(sweep_kernel, True), (*f_left, *forcing, *f_right, inner), [planes], [(2, *tall)], 10**8
    )
    *field, s0, s1, first = call(
        middle_kernel, (*forcing, part, *correction, shift, pairs),
        [chunk] * 4 + [coarse] * 2 + [(1, LANES)], [*scratch, (2, nc, 8, nz), (2, 8, nz)], 10**8,
    )
    (local,) = call(
        rhs_later_kernel, (*forcing, *field, pairs), [coarse], [(1, *tall), (1, nc, 8, nz)], 3 * 10**7
    )
    correction, v_left, v_right, inner = coarse_part(local, s0, s1, 1.0, field, forcing, rows)
    (part,) = call(
        functools.partial(sweep_kernel, False),
        (*v_left, *field, *v_right, *f_left[2:], *f_right[:2], inner), [planes], [(2, *tall)], 10**8,
    )
    result, last = call(
        last_kernel, (*forcing, part, *correction, shift, total, first, pairs),
        [(2, *tiles), (lax.axis_size("gx"), 1, LANES)], [*scratch, (2, 8, nz)], 10**8,
    )
    figures = gathered(last).reshape(-1, LANES)
    blocks = 2
    count = nz // LANES
    result, norms = pl.pallas_call(
        functools.partial(finish_kernel, share),
        grid=(blocks,),
        out_shape=[jax.ShapeDtypeStruct(potential.shape, jnp.float32), jax.ShapeDtypeStruct((CYCLES,), jnp.float32)],
        in_specs=[
            pl.BlockSpec(figures.shape, lambda i: (0, 0)),
            pl.BlockSpec((2, count, ny // blocks, LANES), lambda i: (0, 0, i, 0)),
        ],
        out_specs=[pl.BlockSpec((2, ny // blocks, nz), lambda i: (0, i, 0)), SMEM],
        scratch_shapes=[pltpu.VMEM((8, LANES), jnp.float32)],
        compiler_params=pltpu.CompilerParams(vmem_limit_bytes=16 * 2**20),
        cost_estimate=pl.CostEstimate(flops=10**7, bytes_accessed=8 * result.size, transcendentals=0),
    )(figures, result)
    return (result, norms)


def solution(mesh):
    in_specs = (P(("runs", "gx"), None, None),)
    out_specs = (P(("runs", "gx"), None, None), P("runs"))
    return jax.shard_map(whole, mesh=mesh, in_specs=in_specs, out_specs=out_specs, check_vma=False)
```
